32 devices in a mesh: dp: 16 (over z, y, core), mp: 2 (over x).
Axes of the slice: x: 2, y: 2, z: 4, core: 2. Of those that a mesh axis runs over, the one named last changes fastest.
Arguments:
- images: bfloat16 [64, 196, 512], P('dp'), may hold values from -6 to 6
- loads: int32 [16], P('dp'), may hold values from 1 to 4, as said below
- cotangent: bfloat16 [64, 196, 512], P('dp'), may hold values from -6 to 6
- ln1_gain: float32 [2, 512], replicated, may hold values from 0.5 to 1.5
- ln1_bias: float32 [2, 512], replicated, may hold values from -3 to 3
- w_qkv: bfloat16 [2, 512, 3, 512], P(None, 'dp', None, 'mp'), may hold values from -0.25 to 0.25
- qv_bias: float32 [2, 2, 512], P(None, None, 'mp'), may hold values from -3 to 3
- rel_table: float32 [2, 16, 169], P(None, 'mp'), may hold values from -4 to 330
- w_proj: bfloat16 [2, 512, 512], P(None, 'mp', 'dp'), may hold values from -0.75 to 0.75
- proj_bias: float32 [2, 512], replicated, may hold values from -3 to 3
- ln2_gain: float32 [2, 512], replicated, may hold values from 0.5 to 1.5
- ln2_bias: float32 [2, 512], replicated, may hold values from -3 to 3
- w_fc1: bfloat16 [2, 512, 2048], P(None, 'dp', 'mp'), may hold values from -0.25 to 0.25
- fc1_bias: float32 [2, 2048], P(None, 'mp'), may hold values from -3 to 3
- w_fc2: bfloat16 [2, 2048, 512], P(None, 'mp', 'dp'), may hold values from -0.1875 to 0.1875
- fc2_bias: float32 [2, 512], replicated, may hold values from -3 to 3
Outputs:
- result: bfloat16 [64, 196, 512], P('dp')
- images_grad: bfloat16 [64, 196, 512], P('dp')
- ln1_gain_grad: float32 [2, 512], replicated
- ln1_bias_grad: float32 [2, 512], replicated
- w_qkv_grad: float32 [2, 512, 3, 512], P(None, 'dp', None, 'mp')
- qv_bias_grad: float32 [2, 2, 512], P(None, None, 'mp')
- rel_table_grad: float32 [2, 16, 169], P(None, 'mp')
- w_proj_grad: float32 [2, 512, 512], P(None, 'mp', 'dp')
- proj_bias_grad: float32 [2, 512], replicated
- ln2_gain_grad: float32 [2, 512], replicated
- ln2_bias_grad: float32 [2, 512], replicated
- w_fc1_grad: float32 [2, 512, 2048], P(None, 'dp', 'mp')
- fc1_bias_grad: float32 [2, 2048], P(None, 'mp')
- w_fc2_grad: float32 [2, 2048, 512], P(None, 'mp', 'dp')
- fc2_bias_grad: float32 [2, 512], replicated
The draws below stay inside these ranges and needn't reach their ends.
Inputs may be any that keep to these rules, and one draw needn't show every extreme that they name: `loads`: some index of dp uses all 4 slots.
All inputs are finite; a program needn't handle non-finite values.
Results may differ from the reference program's by a relative error of at most 0.02.
Values may be sent and summed in bfloat16 or wider, within the bound.
A program may use at most 192 MiB of HBM per device.

```python
import jax
import jax.numpy as jnp
from jax import lax

D = 512
HEADS = 16
HD = 32
FF = 2048
SIDE = 14
WIN = 7
SHIFT = 3
LAYERS = 2
IMG_DEV = 4
TOK_IMG = 196
IMAGES = 64
N_DP = 16


def draw_loads(key, part):
    key_one, key_two, key_three = jax.random.split(jax.random.fold_in(key, 5), 3)
    lowest = max(1, IMG_DEV // 3)
    counts = jnp.minimum(jax.random.randint(key_one, (N_DP,), lowest, IMG_DEV + 1), jax.random.randint(key_two, (N_DP,), lowest, IMG_DEV + 1))
    chosen = jax.random.randint(key_three, (), 0, N_DP)
    return counts.at[chosen].set(IMG_DEV).astype(jnp.int32)


def draw_rel_table(key, part):
    key_one = jax.random.fold_in(jax.random.fold_in(key, 11), 0)
    entries = (2 * WIN - 1) ** 2
    shape_all = (LAYERS, HEADS, entries)
    table_vals = jnp.clip(jax.random.normal(key_one, shape_all, jnp.float32), -4.0, 4.0)
    return table_vals


def strengthened(array, key, source, target, blocks, factor):
    owner, partner = [(jnp.arange(array.shape[position]) // (array.shape[position] // blocks)).reshape([-1 if axis == position else 1 for axis in range(array.ndim)]) for position in (source, target)]
    chosen = jax.random.permutation(key, blocks)[partner]
    strong = (owner == chosen) | (owner == (partner + blocks // 2) % blocks)
    return jnp.where(strong, factor * array, array)


def steps_of(rng, shape, cuts, least, high):
    level = 1.0
    for position, blocks in cuts:
        draws = jax.random.uniform(jax.random.fold_in(jax.random.fold_in(rng, 6), position), (blocks,), jnp.float32, least / len(cuts), high / len(cuts))
        level = level * jnp.repeat(jnp.exp(draws), shape[position] // blocks).reshape((-1,) + (1,) * (len(shape) - 1 - position))
    return level


def noise(own_key, dims, deviation, reach, pieces=(), kind=jnp.bfloat16):
    values = jax.random.normal(own_key, dims, jnp.float32) * deviation
    if len(pieces) > 0:
        values = steps_of(own_key, dims, pieces, -0.22, 0.18) * values
    return jnp.clip(values, min=-reach, max=reach).astype(kind)


def heavy_noise(rng, dims, width, bound, pieces, heavy, held_as=jnp.bfloat16):
    array = width * jax.random.normal(rng, dims, jnp.float32)
    if pieces:
        array = array * steps_of(rng, dims, pieces, -0.22, 0.18)
    return jnp.clip(strengthened(array, jax.random.fold_in(rng, 3), *heavy), -bound, bound).astype(held_as)


def setup_inputs(seed: int = 0) -> dict:
    key_list = jax.random.split(jax.random.key(seed), 17)
    images = heavy_noise(key_list[0], (IMAGES, TOK_IMG, D), 1.0, 6.0, ((0, 16),), (0, 2, 16, 2.0))
    loads = draw_loads(jax.random.fold_in(key_list[16], 71), 0)
    cotangent = heavy_noise(key_list[2], (IMAGES, TOK_IMG, D), 1.0, 6.0, ((0, 16),), (0, 2, 16, 2.0))
    ln1_gain = jnp.clip(1.0 + 0.1 * jax.random.normal(key_list[3], (LAYERS, D), jnp.float32), 0.5, 1.5)
    ln1_bias = noise(key_list[4], (LAYERS, D), 0.5, 3.0, (), jnp.float32)
    w_qkv = noise(key_list[5], (LAYERS, D, 3, D), D ** -0.5, 0.25, ((1, 16), (3, 2)))
    qv_bias = noise(key_list[6], (LAYERS, 2, D), 0.5, 3.0, ((2, 2),), jnp.float32)
    rel_table = draw_rel_table(jax.random.fold_in(key_list[16], 71), 0)
    w_proj = noise(key_list[8], (LAYERS, D, D), (D // 8) ** -0.5, 0.75, ((1, 2), (2, 16)))
    proj_bias = noise(key_list[9], (LAYERS, D), 0.5, 3.0, (), jnp.float32)
    ln2_gain = jnp.clip(1.0 + 0.1 * jax.random.normal(key_list[10], (LAYERS, D), jnp.float32), 0.5, 1.5)
    ln2_bias = noise(key_list[11], (LAYERS, D), 0.5, 3.0, (), jnp.float32)
    w_fc1 = noise(key_list[12], (LAYERS, D, FF), D ** -0.5, 0.25, ((1, 16), (2, 2)))
    fc1_bias = noise(key_list[13], (LAYERS, FF), 0.5, 3.0, ((1, 2),), jnp.float32)
    w_fc2 = noise(key_list[14], (LAYERS, FF, D), (FF // 2) ** -0.5, 0.1875, ((1, 2), (2, 16)))
    fc2_bias = noise(key_list[15], (LAYERS, D), 0.5, 3.0, (), jnp.float32)
    return {"images": images, "loads": loads, "cotangent": cotangent, "ln1_gain": ln1_gain, "ln1_bias": ln1_bias, "w_qkv": w_qkv, "qv_bias": qv_bias, "rel_table": rel_table, "w_proj": w_proj, "proj_bias": proj_bias, "ln2_gain": ln2_gain, "ln2_bias": ln2_bias, "w_fc1": w_fc1, "fc1_bias": fc1_bias, "w_fc2": w_fc2, "fc2_bias": fc2_bias}


EPS = 1e-05
MASKED = -1e+30
INV_ROOT_TWO = 0.7071067811865476
INV_ROOT_TWOPI = 0.3989422804014327

def offsets_table():
    cells = jnp.arange(WIN * WIN, dtype=jnp.int32)
    rows_at = cells // WIN
    cols_at = cells % WIN
    index_all = (rows_at[:, None] - rows_at[None, :] + WIN - 1) * (2 * WIN - 1) + (cols_at[:, None] - cols_at[None, :] + WIN - 1)
    entries = jnp.arange((2 * WIN - 1) ** 2, dtype=jnp.int32)
    return (index_all.reshape(-1)[:, None] == entries[None, :]).astype(jnp.float32)

def window_cut(token_grid):
    image_count = token_grid.shape[0]
    tail_dims = token_grid.shape[3:]
    per_side = SIDE // WIN
    token_grid = token_grid.reshape((image_count, per_side, WIN, per_side, WIN) + tail_dims)
    token_grid = jnp.moveaxis(token_grid, 3, 2)
    return token_grid.reshape((image_count * per_side * per_side, WIN * WIN) + tail_dims)

def window_paste(windows, image_count):
    per_side = SIDE // WIN
    tail_dims = windows.shape[2:]
    token_grid = windows.reshape((image_count, per_side, per_side, WIN, WIN) + tail_dims)
    token_grid = jnp.moveaxis(token_grid, 2, 3)
    return token_grid.reshape((image_count, SIDE, SIDE) + tail_dims)

def window_split(token_rows, image_count, shifted):
    token_grid = token_rows.reshape((image_count, SIDE, SIDE) + token_rows.shape[1:])
    if shifted:
        token_grid = jnp.roll(token_grid, (-SHIFT, -SHIFT), (1, 2))
    return window_cut(token_grid)

def window_join(windows, image_count, shifted):
    token_grid = window_paste(windows, image_count)
    if shifted:
        token_grid = jnp.roll(token_grid, (SHIFT, SHIFT), (1, 2))
    return token_grid.reshape((image_count * SIDE * SIDE,) + token_grid.shape[3:])

def region_match():
    line_at = jnp.arange(SIDE, dtype=jnp.int32)
    band_at = jnp.where(line_at < SIDE - WIN, 0, jnp.where(line_at < SIDE - SHIFT, 1, 2))
    region = band_at[:, None] * 3 + band_at[None, :]
    region_win = window_cut(region[None])
    return region_win[:, :, None] == region_win[:, None, :]

def head_bias(offsets, table_vals):
    flat = jnp.dot(offsets, table_vals.T, precision=lax.Precision.HIGHEST)
    return flat.reshape(WIN * WIN, WIN * WIN, -1).transpose(2, 0, 1)

def score_block(query_win, key_win, bias_heads, same_region, image_count, shifted):
    scores = jnp.einsum('wihd,wjhd->whij', query_win.astype(jnp.float32), key_win.astype(jnp.float32)) + bias_heads[None]
    if shifted:
        scores = scores.reshape((image_count, -1) + scores.shape[1:])
        scores = jnp.where(same_region[None, :, None], scores, MASKED)
        scores = scores.reshape((-1,) + scores.shape[2:])
    return scores

def normalize(stream):
    centre = stream - lax.optimization_barrier(jnp.mean(stream, -1, keepdims=True))
    rstd = lax.rsqrt(lax.optimization_barrier(jnp.mean(centre * centre, -1, keepdims=True)) + EPS)
    return (centre * rstd, rstd)

def normalize_back(grad_y, normed, rstd, gain):
    gain_grad = lax.optimization_barrier(jnp.sum(grad_y * normed, 0))
    shift_grad = lax.optimization_barrier(jnp.sum(grad_y, 0))
    scaled = grad_y * gain
    grad_x = rstd * (scaled - lax.optimization_barrier(jnp.mean(scaled, -1, keepdims=True)) - normed * lax.optimization_barrier(jnp.mean(scaled * normed, -1, keepdims=True)))
    return (grad_x, gain_grad, shift_grad)

def gelu_slope(pre_act):
    return 0.5 * (1.0 + lax.erf(pre_act * INV_ROOT_TWO)) + pre_act * jnp.exp(-0.5 * pre_act * pre_act) * INV_ROOT_TWOPI

def attend_forward(inputs_a, w_mix, mix_bias, table_vals, image_count, shifted, offsets, same_region):
    local_width = w_mix.shape[2]
    head_count = table_vals.shape[0]
    mixed_qkv = jnp.dot(inputs_a, w_mix.reshape(w_mix.shape[0], 3 * local_width), preferred_element_type=jnp.float32).reshape(-1, 3, local_width)
    scale_q = HD ** (-0.5)
    query_rows = ((mixed_qkv[:, 0] + mix_bias[0]) * scale_q).astype(jnp.bfloat16)
    key_rows = mixed_qkv[:, 1].astype(jnp.bfloat16)
    value_rows = (mixed_qkv[:, 2] + mix_bias[1]).astype(jnp.bfloat16)
    query_win = window_split(query_rows.reshape(-1, head_count, HD), image_count, shifted)
    key_win = window_split(key_rows.reshape(-1, head_count, HD), image_count, shifted)
    value_win = window_split(value_rows.reshape(-1, head_count, HD), image_count, shifted)
    bias_heads = head_bias(offsets, table_vals)
    scores = score_block(query_win, key_win, bias_heads, same_region, image_count, shifted)
    row_max = lax.optimization_barrier(jnp.max(scores, -1, keepdims=True))
    log_total = row_max + jnp.log(lax.optimization_barrier(jnp.sum(jnp.exp(scores - row_max), -1, keepdims=True)))
    probs = jnp.exp(scores - log_total).astype(jnp.bfloat16)
    attended_win = jnp.einsum('whij,wjhd->wihd', probs.astype(jnp.float32), value_win.astype(jnp.float32)).astype(jnp.bfloat16)
    attended = window_join(attended_win, image_count, shifted).reshape(-1, local_width)
    return (attended, (query_win, key_win, value_win, log_total))

def attend_backward(att_grad, attn_keep, inputs_a, w_mix, table_vals, image_count, shifted, offsets, same_region):
    query_win, key_win, value_win, log_total = attn_keep
    local_width = w_mix.shape[2]
    head_count = table_vals.shape[0]
    scale_q = HD ** (-0.5)
    grad_win = window_split(att_grad.reshape(-1, head_count, HD), image_count, shifted)
    bias_heads = head_bias(offsets, table_vals)
    scores = score_block(query_win, key_win, bias_heads, same_region, image_count, shifted)
    probs_f = jnp.exp(scores - log_total)
    probs = probs_f.astype(jnp.bfloat16)
    value_grad = jnp.einsum('whij,wihd->wjhd', probs.astype(jnp.float32), grad_win.astype(jnp.float32))
    prob_grad = jnp.einsum('wihd,wjhd->whij', grad_win.astype(jnp.float32), value_win.astype(jnp.float32))
    row_dot = lax.optimization_barrier(jnp.sum(probs_f * prob_grad, -1, keepdims=True))
    score_grad = probs_f * (prob_grad - row_dot)
    table_grad = jnp.dot(lax.optimization_barrier(jnp.sum(score_grad, 0)).reshape(head_count, -1), offsets, precision=lax.Precision.HIGHEST)
    score_low = score_grad.astype(jnp.bfloat16)
    query_grad = jnp.einsum('whij,wjhd->wihd', score_low.astype(jnp.float32), key_win.astype(jnp.float32)) * scale_q
    key_grad = jnp.einsum('whij,wihd->wjhd', score_low.astype(jnp.float32), query_win.astype(jnp.float32))
    query_rows = window_join(query_grad, image_count, shifted).reshape(-1, local_width)
    key_rows = window_join(key_grad, image_count, shifted).reshape(-1, local_width)
    value_rows = window_join(value_grad, image_count, shifted).reshape(-1, local_width)
    mix_bias_grad = jnp.stack([lax.optimization_barrier(jnp.sum(query_rows, 0)), lax.optimization_barrier(jnp.sum(value_rows, 0))])
    mix_grad = jnp.stack([query_rows, key_rows, value_rows], 1).astype(jnp.bfloat16).reshape(-1, 3 * local_width)
    w_mix_grad = jnp.dot(inputs_a.T, mix_grad, preferred_element_type=jnp.float32).reshape(w_mix.shape)
    input_grad = jnp.dot(mix_grad, w_mix.reshape(w_mix.shape[0], -1).T, preferred_element_type=jnp.float32)
    return (w_mix_grad, mix_bias_grad, table_grad, input_grad)

def forward_layer(stream, weights, image_count, shifted, offsets, same_region):
    gain_a, shift_a, w_mix, mix_bias, table_vals, w_out, out_bias, gain_b, shift_b, w_up, up_bias, w_down, down_bias = weights
    normed_a, rstd_a = normalize(stream)
    inputs_a = (normed_a * gain_a + shift_a).astype(jnp.bfloat16)
    attended, attn_keep = attend_forward(inputs_a, w_mix, mix_bias, table_vals, image_count, shifted, offsets, same_region)
    middle = stream + jnp.dot(attended, w_out, preferred_element_type=jnp.float32) + out_bias
    normed_b, rstd_b = normalize(middle)
    inputs_b = (normed_b * gain_b + shift_b).astype(jnp.bfloat16)
    pre_act = jnp.dot(inputs_b, w_up, preferred_element_type=jnp.float32) + up_bias
    activated = jax.nn.gelu(pre_act, approximate=False).astype(jnp.bfloat16)
    stream_next = middle + jnp.dot(activated, w_down, preferred_element_type=jnp.float32) + down_bias
    return (stream_next, (inputs_a, normed_a, rstd_a, attn_keep, attended, normed_b, rstd_b, inputs_b, pre_act, activated))

def backward_layer(grad_flow, keep, weights, image_count, shifted, offsets, same_region):
    gain_a, shift_a, w_mix, mix_bias, table_vals, w_out, out_bias, gain_b, shift_b, w_up, up_bias, w_down, down_bias = weights
    inputs_a, normed_a, rstd_a, attn_keep, attended, normed_b, rstd_b, inputs_b, pre_act, activated = keep
    down_bias_grad = lax.optimization_barrier(jnp.sum(grad_flow, 0))
    grad_low = grad_flow.astype(jnp.bfloat16)
    w_down_grad = jnp.dot(activated.T, grad_low, preferred_element_type=jnp.float32)
    act_grad = jnp.dot(grad_low, w_down.T, preferred_element_type=jnp.float32)
    pre_grad = act_grad * gelu_slope(pre_act)
    up_bias_grad = lax.optimization_barrier(jnp.sum(pre_grad, 0))
    pre_low = pre_grad.astype(jnp.bfloat16)
    w_up_grad = jnp.dot(inputs_b.T, pre_low, preferred_element_type=jnp.float32)
    inputs_b_grad = jnp.dot(pre_low, w_up.T, preferred_element_type=jnp.float32)
    mid_grad, gain_b_grad, shift_b_grad = normalize_back(inputs_b_grad, normed_b, rstd_b, gain_b)
    mid_grad = mid_grad + grad_flow
    out_bias_grad = lax.optimization_barrier(jnp.sum(mid_grad, 0))
    mid_low = mid_grad.astype(jnp.bfloat16)
    w_out_grad = jnp.dot(attended.T, mid_low, preferred_element_type=jnp.float32)
    att_grad = jnp.dot(mid_low, w_out.T, preferred_element_type=jnp.float32).astype(jnp.bfloat16)
    w_mix_grad, mix_bias_grad, table_grad, inputs_a_grad = attend_backward(att_grad, attn_keep, inputs_a, w_mix, table_vals, image_count, shifted, offsets, same_region)
    stream_grad, gain_a_grad, shift_a_grad = normalize_back(inputs_a_grad, normed_a, rstd_a, gain_a)
    stream_grad = stream_grad + mid_grad
    return (stream_grad, (gain_a_grad, shift_a_grad, w_mix_grad, mix_bias_grad, table_grad, w_out_grad, out_bias_grad, gain_b_grad, shift_b_grad, w_up_grad, up_bias_grad, w_down_grad, down_bias_grad))

def reference(images, loads, cotangent, ln1_gain, ln1_bias, w_qkv, qv_bias, rel_table, w_proj, proj_bias, ln2_gain, ln2_bias, w_fc1, fc1_bias, w_fc2, fc2_bias):
    params = (ln1_gain, ln1_bias, w_qkv, qv_bias, rel_table, w_proj, proj_bias, ln2_gain, ln2_bias, w_fc1, fc1_bias, w_fc2, fc2_bias)
    offsets = offsets_table()
    same_region = region_match()
    image_blocks = images.reshape(N_DP, IMG_DEV, TOK_IMG, D)
    cot_blocks = cotangent.reshape(N_DP, IMG_DEV, TOK_IMG, D)

    def one_device(totals, inputs):
        image_block, load_now, cot_block = inputs
        slot_valid = (jnp.arange(IMG_DEV, dtype=jnp.int32) < load_now).astype(jnp.float32)
        row_valid = jnp.repeat(slot_valid, TOK_IMG)[:, None]
        stream = image_block.reshape(-1, D).astype(jnp.float32)
        keeps = []
        for layer_at in range(LAYERS):
            weights = tuple((member[layer_at] for member in params))
            stream, keep = forward_layer(stream, weights, IMG_DEV, layer_at % 2 == 1, offsets, same_region)
            keeps.append(keep)
        output = (stream * row_valid).astype(jnp.bfloat16).reshape(IMG_DEV, TOK_IMG, D)
        grad_flow = cot_block.reshape(-1, D).astype(jnp.float32) * row_valid
        layer_grads = [None] * LAYERS
        for layer_at in reversed(range(LAYERS)):
            weights = tuple((member[layer_at] for member in params))
            grad_flow, layer_grads[layer_at] = backward_layer(grad_flow, keeps[layer_at], weights, IMG_DEV, layer_at % 2 == 1, offsets, same_region)
        stacked = tuple((jnp.stack([layer_grads[layer_at][member] for layer_at in range(LAYERS)]) for member in range(len(params))))
        totals = tuple((total + part_sum for total, part_sum in zip(totals, stacked)))
        return (totals, (output, grad_flow.astype(jnp.bfloat16).reshape(IMG_DEV, TOK_IMG, D)))
    initial = tuple((jnp.zeros(member.shape, jnp.float32) for member in params))
    totals, (outputs, input_grads) = lax.scan(one_device, initial, (image_blocks, loads, cot_blocks))
    result = outputs.reshape(IMAGES, TOK_IMG, D)
    images_grad = input_grads.reshape(IMAGES, TOK_IMG, D)
    return (result, images_grad, totals[0], totals[1], totals[2], totals[3], totals[4], totals[5], totals[6], totals[7], totals[8], totals[9], totals[10], totals[11], totals[12])
```

```python
import functools
import types

import jax
import jax.numpy as jnp
import numpy as np
from jax import lax
from jax.experimental import pallas as pl
from jax.experimental.pallas import tpu as pltpu
from jax.sharding import PartitionSpec as P

D = 512
HD = 32
FF = 2048
SIDE = 14
WIN = 7
SHIFT = 3
LAYERS = 2
TOK_IMG = SIDE * SIDE
CELLS = WIN * WIN
PADC = 64
EPS = 1e-05
MASKED = -1e30
INV_ROOT_TWO = 0.7071067811865476
INV_ROOT_TWOPI = 0.3989422804014327
SCALE_Q = HD**-0.5

OWN = 2
ROWS = 400
WROWS = OWN * 4 * PADC
STEP = 80
HALF = 256
F32 = jnp.float32
BF16 = jnp.bfloat16


def token_maps():
    idx = np.full((LAYERS, WROWS), -1, np.int32)
    reg = np.zeros((LAYERS, 4, PADC), np.int32)
    for layer in range(LAYERS):
        shift = SHIFT if layer % 2 else 0
        for win in range(OWN * 4):
            img, wr, wc = win // 4, (win // 2) % 2, win % 2
            for cell in range(CELLS):
                r, c = wr * WIN + cell // WIN, wc * WIN + cell % WIN
                idx[layer, win * PADC + cell] = (
                    img * TOK_IMG + ((r + shift) % SIDE) * SIDE + (c + shift) % SIDE
                )
                if shift:
                    band = lambda v: 0 if v < SIDE - WIN else (1 if v < SIDE - SHIFT else 2)
                    reg[layer, win % 4, cell] = 3 * band(r) + band(c)
    return idx, reg


def bias_onehot():
    cells = np.arange(CELLS)
    r, c = cells // WIN, cells % WIN
    entry = (r[None, :] - r[:, None] + WIN - 1) * (2 * WIN - 1) + (
        c[None, :] - c[:, None] + WIN - 1
    )
    full = np.full((PADC, PADC), -1, np.int32)
    full[:CELLS, :CELLS] = entry
    return full


def dot(a, b):
    return jnp.dot(a, b, preferred_element_type=F32)


def dot_nt(a, b):
    return lax.dot_general(a, b, (((1,), (1,)), ((), ())), preferred_element_type=F32)


def dot_tn(a, b):
    return lax.dot_general(a, b, (((0,), (0,)), ((), ())), preferred_element_type=F32)


def lane_head(shape):
    return lax.broadcasted_iota(jnp.int32, shape, 1) // HD


def spread_heads(block):
    head = lane_head(block.shape)
    zero = jnp.zeros_like(block)
    return jnp.concatenate([jnp.where(head == h, block, zero) for h in range(4)], axis=0)


def gather_heads(stack):
    head = lane_head((PADC, 128))
    total = jnp.where(head == 0, stack[:PADC], 0.0)
    for h in range(1, 4):
        total = total + jnp.where(head == h, stack[h * PADC : (h + 1) * PADC], 0.0)
    return total


def row_loop(body, init):
    def step(i, carry):
        return body(pl.ds(pl.multiple_of(i * STEP, STEP), STEP), carry)

    return lax.fori_loop(0, ROWS // STEP, step, init)


def weight(r, l, g, x, cols):
    part = r.W[l, g, x, :, :, cols]
    return part.reshape(D, part.shape[-1])


def weight_rows(r, l, g, x, n, cols):
    per = HALF // r.W.shape[4]
    part = r.W[l, g, x, pl.ds(n * per, per), :, cols]
    return part.reshape(HALF, part.shape[-1])


def put_grad(r, l, g, x, cols, value):
    z, rb = r.G.shape[3], r.G.shape[4]
    r.G[l, g, x, :, :, cols] = value.astype(BF16).reshape(z, rb, value.shape[-1])


def norm_into(r, l, src, normed, rstd_ref, gain, shift, out):
    def body(rows, carry):
        s = src[rows, :]
        centre = s - jnp.mean(s, -1, keepdims=True)
        rstd = lax.rsqrt(jnp.mean(centre * centre, -1, keepdims=True) + EPS)
        n = centre * rstd
        normed[l, rows, :] = n
        rstd_ref[l, rows, :] = rstd
        out[rows, :] = (n * gain[l] + shift[l]).astype(BF16)
        return carry

    row_loop(body, 0)


def norm_back(r, l, grad_y, normed, rstd_ref, gain, base, out, out_low):
    def body(rows, carry):
        gain_sum, shift_sum, out_sum = carry
        gy = grad_y[rows, :]
        n = normed[l, rows, :]
        e = gy * gain[l]
        back = rstd_ref[l, rows, :] * (
            e - jnp.mean(e, -1, keepdims=True) - n * jnp.mean(e * n, -1, keepdims=True)
        )
        res = base[rows, :] + back
        out[rows, :] = res
        out_low[rows, :] = res.astype(BF16)
        return (
            gain_sum + jnp.sum(gy * n, 0, keepdims=True),
            shift_sum + jnp.sum(gy, 0, keepdims=True),
            out_sum + jnp.sum(res, 0, keepdims=True),
        )

    zero = jnp.zeros((1, D), F32)
    return row_loop(body, (zero, zero, zero))


def to_windows(r, l):
    tok = lax.broadcasted_iota(jnp.int32, (WROWS, ROWS), 1)
    return jnp.where(tok == r.idx_col[l], 1.0, 0.0).astype(BF16)


def to_grid(r, l):
    tok = lax.broadcasted_iota(jnp.int32, (ROWS, WROWS), 0)
    return jnp.where(tok == r.idx_row[l], 1.0, 0.0).astype(BF16)


def attention_forward(r, l):
    def window(w, carry):
        rows = pl.ds(pl.multiple_of(w * PADC, PADC), PADC)
        pos = lax.rem(w, 4)
        same = r.reg_col[l, pos] == r.reg_row[l, pos]
        for g in range(4):
            lanes = slice(g * 128, (g + 1) * 128)
            q, k, v = r.Q[l, rows, lanes], r.K[l, rows, lanes], r.V[l, rows, lanes]
            s = dot_nt(k, spread_heads(q)) + r.bias[l, g]
            s = jnp.where(same, s, MASKED)
            e = jnp.exp(s - jnp.max(s, 0, keepdims=True))
            p = (e / jnp.sum(e, 0, keepdims=True)).astype(BF16)
            r.PR[l, w * 4 + g] = p
            r.AW[rows, lanes] = gather_heads(dot_tn(p, v)).astype(BF16)
        return carry

    lax.fori_loop(0, OWN * 4, window, 0)


def attention_backward(r, l):
    zero = jnp.zeros((1, 128), F32)

    def window(w, carry):
        rows = pl.ds(pl.multiple_of(w * PADC, PADC), PADC)
        sums = list(carry)
        for g in range(4):
            lanes = slice(g * 128, (g + 1) * 128)
            q, k, v = r.Q[l, rows, lanes], r.K[l, rows, lanes], r.V[l, rows, lanes]
            da = r.AW[rows, lanes]
            p = r.PR[l, w * 4 + g]
            da_spread = spread_heads(da)
            pf = p.astype(F32)
            pg = dot_nt(v, da_spread)
            ds = pf * (pg - jnp.sum(pf * pg, 0, keepdims=True))
            r.DS[l, g] += ds
            low = ds.astype(BF16)
            dv = dot(p, da_spread)
            dk = dot(low, spread_heads(q))
            dq = gather_heads(dot_tn(low, k)) * SCALE_Q
            x, at = g // 2, (g % 2) * 128
            r.DM[x, rows, at : at + 128] = dq.astype(BF16)
            r.DM[x, rows, HALF + at : HALF + at + 128] = dk.astype(BF16)
            r.DM[x, rows, 2 * HALF + at : 2 * HALF + at + 128] = dv.astype(BF16)
            sums[g] = sums[g] + jnp.sum(dq, 0, keepdims=True)
            sums[4 + g] = sums[4 + g] + jnp.sum(dv, 0, keepdims=True)
        return tuple(sums)

    return lax.fori_loop(0, OWN * 4, window, (zero,) * 8)


def forward(r, l):
    norm_into(r, l, r.S, r.N1, r.R1, r.ln1_gain, r.ln1_bias, r.YB)
    r.YW[l] = dot(to_windows(r, l), r.YB[...]).astype(BF16)
    yw = r.YW[l]
    for x in range(2):
        cols = slice(x * HALF, (x + 1) * HALF)
        q = dot(yw, weight(r, l, 0, x, slice(0, HALF)))
        r.Q[l, :, cols] = ((q + r.qv_bias[l, 0:1, cols]) * SCALE_Q).astype(BF16)
        r.K[l, :, cols] = dot(yw, weight(r, l, 0, x, slice(HALF, 2 * HALF))).astype(BF16)
        v = dot(yw, weight(r, l, 0, x, slice(2 * HALF, 3 * HALF)))
        r.V[l, :, cols] = (v + r.qv_bias[l, 1:2, cols]).astype(BF16)
    attention_forward(r, l)
    r.AT[l] = dot(to_grid(r, l), r.AW[...]).astype(BF16)
    for n in range(2):
        cols = slice(n * HALF, (n + 1) * HALF)
        acc = dot_nt(r.AT[l, :, :HALF], weight_rows(r, l, 0, 0, n, slice(3 * HALF, 4 * HALF)))
        acc += dot_nt(r.AT[l, :, HALF:], weight_rows(r, l, 0, 1, n, slice(3 * HALF, 4 * HALF)))
        r.S[:, cols] = r.S[:, cols] + acc + r.proj_bias[l, :, cols]
    norm_into(r, l, r.S, r.N2, r.R2, r.ln2_gain, r.ln2_bias, r.YB)
    r.Y2[l] = r.YB[...]
    for x in range(2):

        def up(n, carry):
            at = pl.ds(pl.multiple_of(n * HALF, HALF), HALF)
            full = pl.ds(pl.multiple_of(x * 1024 + n * HALF, HALF), HALF)
            pre = dot(r.YB[...], weight(r, l, 1, x, at)) + r.fc1_bias[l, :, full]
            phi = 0.5 * (1.0 + lax.erf(pre * INV_ROOT_TWO))
            r.AC[l, :, full] = (pre * phi).astype(BF16)
            dens = jnp.exp(-0.5 * pre * pre) * INV_ROOT_TWOPI
            r.SL[l, :, full] = (phi + pre * dens).astype(BF16)
            return carry

        lax.fori_loop(0, 4, up, 0)
    for n in range(2):
        cols = slice(n * HALF, (n + 1) * HALF)
        acc = dot_nt(r.AC[l, :, :1024], weight_rows(r, l, 2, 0, n, slice(0, 1024)))
        acc += dot_nt(r.AC[l, :, 1024:], weight_rows(r, l, 2, 1, n, slice(0, 1024)))
        r.S[:, cols] = r.S[:, cols] + acc + r.fc2_bias[l, :, cols]


def backward_mlp(r, l):
    def low(rows, total):
        g = r.S[rows, :]
        r.YB[rows, :] = g.astype(BF16)
        return total + jnp.sum(g, 0, keepdims=True)

    r.SG[l, 2:3, D : 2 * D] = row_loop(low, jnp.zeros((1, D), F32))
    r.TA[...] = r.YB[...].T
    r.TB[...] = r.Y2[l].T
    for x in range(2):

        def down(n, carry):
            at = pl.ds(pl.multiple_of(n * HALF, HALF), HALF)
            full = pl.ds(pl.multiple_of(x * 1024 + n * HALF, HALF), HALF)
            pg = dot(r.YB[...], weight(r, l, 2, x, at)) * r.SL[l, :, full].astype(F32)
            r.SG[l, 0:1, full] = jnp.sum(pg, 0, keepdims=True)
            pb = pg.astype(BF16)
            r.PB[:, full] = pb
            put_grad(r, l, 2, x, at, dot(r.TA[...], r.AC[l, :, full]))
            put_grad(r, l, 1, x, at, dot(r.TB[...], pb))
            return carry

        lax.fori_loop(0, 4, down, 0)
    for n in range(2):
        cols = slice(n * HALF, (n + 1) * HALF)
        acc = dot_nt(r.PB[:, :1024], weight_rows(r, l, 1, 0, n, slice(0, 1024)))
        acc += dot_nt(r.PB[:, 1024:], weight_rows(r, l, 1, 1, n, slice(0, 1024)))
        r.GY[:, cols] = acc
    gain, shift, out = norm_back(r, l, r.GY, r.N2, r.R2, r.ln2_gain, r.S, r.S, r.YB)
    r.SG[l, 1:2, 2 * D : 3 * D] = gain
    r.SG[l, 1:2, 3 * D :] = shift
    r.SG[l, 2:3, :D] = out


def backward_attention(r, l):
    r.TA[...] = r.YB[...].T
    for x in range(2):
        cols = slice(x * HALF, (x + 1) * HALF)
        put_grad(r, l, 0, x, slice(3 * HALF, 4 * HALF), dot(r.TA[...], r.AT[l, :, cols]))
        att = dot(r.YB[...], weight(r, l, 0, x, slice(3 * HALF, 4 * HALF)))
        r.GB[:, cols] = att.astype(BF16)
    r.AW[...] = dot(to_windows(r, l), r.GB[...]).astype(BF16)
    r.DS[l] = jnp.zeros_like(r.DS[l])
    sums = attention_backward(r, l)
    for g in range(4):
        r.SG[l, 2:3, 2 * D + g * 128 : 2 * D + (g + 1) * 128] = sums[g]
        r.SG[l, 2:3, 3 * D + g * 128 : 3 * D + (g + 1) * 128] = sums[4 + g]
    r.TW[...] = r.YW[l].T
    for x in range(2):
        for part in range(3):
            cols = slice(part * HALF, (part + 1) * HALF)
            put_grad(r, l, 0, x, cols, dot(r.TW[...], r.DM[x, :, cols]))
    for n in range(2):
        cols = slice(n * HALF, (n + 1) * HALF)
        acc = dot_nt(r.DM[0], weight_rows(r, l, 0, 0, n, slice(0, 3 * HALF)))
        acc += dot_nt(r.DM[1], weight_rows(r, l, 0, 1, n, slice(0, 3 * HALF)))
        r.AW[:, cols] = acc.astype(BF16)
    r.GY[...] = dot(to_grid(r, l), r.AW[...])
    gain, shift, _ = norm_back(r, l, r.GY, r.N1, r.R1, r.ln1_gain, r.S, r.S, r.YB)
    r.SG[l, 1:2, :D] = gain
    r.SG[l, 1:2, D : 2 * D] = shift


INPUTS = (
    "x", "cot", "valid", "idx_col", "idx_row", "reg_col", "reg_row", "bias",
    "ln1_gain", "ln1_bias", "qv_bias", "proj_bias", "ln2_gain", "ln2_bias", "fc1_bias", "fc2_bias",
)
SMALL_ROWS = 8


def scratch_spec():
    return dict(
        S=pltpu.VMEM((ROWS, D), F32),
        GY=pltpu.VMEM((ROWS, D), F32),
        YB=pltpu.VMEM((ROWS, D), BF16),
        GB=pltpu.VMEM((ROWS, D), BF16),
        N1=pltpu.VMEM((LAYERS, ROWS, D), F32),
        N2=pltpu.VMEM((LAYERS, ROWS, D), F32),
        R1=pltpu.VMEM((LAYERS, ROWS, 1), F32),
        R2=pltpu.VMEM((LAYERS, ROWS, 1), F32),
        YW=pltpu.VMEM((LAYERS, WROWS, D), BF16),
        Q=pltpu.VMEM((LAYERS, WROWS, D), BF16),
        K=pltpu.VMEM((LAYERS, WROWS, D), BF16),
        V=pltpu.VMEM((LAYERS, WROWS, D), BF16),
        PR=pltpu.VMEM((LAYERS, OWN * 16, PADC, 4 * PADC), BF16),
        AW=pltpu.VMEM((WROWS, D), BF16),
        AT=pltpu.VMEM((LAYERS, ROWS, D), BF16),
        Y2=pltpu.VMEM((LAYERS, ROWS, D), BF16),
        AC=pltpu.VMEM((LAYERS, ROWS, FF), BF16),
        SL=pltpu.VMEM((LAYERS, ROWS, FF), BF16),
        PB=pltpu.VMEM((ROWS, FF), BF16),
        DM=pltpu.VMEM((2, WROWS, 3 * HALF), BF16),
        TA=pltpu.VMEM((D, ROWS), BF16),
        TB=pltpu.VMEM((D, ROWS), BF16),
        TW=pltpu.VMEM((D, WROWS), BF16),
    )


def compute_kernel(names, *refs):
    r = types.SimpleNamespace(**dict(zip(names, refs)))
    r.S[...] = r.x[...].astype(F32)
    lax.fori_loop(0, LAYERS, lambda l, c: (forward(r, l), c)[1], 0)
    r.result[...] = (r.S[...] * r.valid[...]).astype(BF16)
    r.S[...] = r.cot[...].astype(F32) * r.valid[...]

    def back(i, c):
        l = LAYERS - 1 - i
        backward_mlp(r, l)
        backward_attention(r, l)
        return c

    lax.fori_loop(0, LAYERS, back, 0)
    r.gimg[...] = r.YB[...]


def compute_call(ins, w):
    z, rb = w.shape[3], w.shape[4]
    outs = dict(
        G=jax.ShapeDtypeStruct((LAYERS, 3, 2, z, rb, 1024), BF16),
        SG=jax.ShapeDtypeStruct((LAYERS, SMALL_ROWS, FF), F32),
        DS=jax.ShapeDtypeStruct((LAYERS, 4, PADC, 4 * PADC), F32),
        result=jax.ShapeDtypeStruct((ROWS, D), BF16),
        gimg=jax.ShapeDtypeStruct((ROWS, D), BF16),
    )
    scratch = scratch_spec()
    names = INPUTS + ("W",) + tuple(outs) + tuple(scratch)
    got = pl.pallas_call(
        functools.partial(compute_kernel, names),
        out_shape=list(outs.values()),
        in_specs=[pl.BlockSpec(memory_space=pltpu.VMEM)] * (len(INPUTS) + 1),
        out_specs=[pl.BlockSpec(memory_space=pltpu.VMEM)] * len(outs),
        scratch_shapes=list(scratch.values()),
        compiler_params=pltpu.CompilerParams(vmem_limit_bytes=67043328),
        name="step",
    )(*[ins[name] for name in INPUTS], w)
    return dict(zip(outs, got))


def small_inputs(images, cot, load, mp, smalls):
    idx, reg = token_maps()
    keep = OWN * TOK_IMG

    def own(arr):
        rows = lax.dynamic_slice_in_dim(arr.reshape(-1, D), mp * keep, keep, 0)
        return jnp.pad(rows, ((0, ROWS - keep), (0, 0)))

    slot = mp * OWN + jnp.arange(ROWS, dtype=jnp.int32) // TOK_IMG
    live = (slot < load) & (jnp.arange(ROWS) < keep)
    ln1_gain, ln1_bias, qv_bias, rel_table, proj_bias, ln2_gain, ln2_bias, fc1_bias, fc2_bias = smalls
    heads = rel_table.shape[1]
    entries = rel_table.shape[2]
    entry = jnp.asarray(bias_onehot().reshape(-1))
    onehot = (entry[:, None] == jnp.arange(entries, dtype=jnp.int32)[None, :]).astype(F32)
    flat = lax.dot_general(
        onehot, rel_table.reshape(LAYERS * heads, entries), (((1,), (1,)), ((), ())),
        precision=lax.Precision.HIGHEST,
    )
    bias = flat.reshape(PADC, PADC, LAYERS, heads // 4, 4).transpose(2, 3, 0, 4, 1)
    pad_key = jnp.arange(PADC)[:, None, None] >= CELLS
    bias = jnp.where(pad_key, MASKED, bias).reshape(LAYERS, heads // 4, PADC, 4 * PADC)
    row = lambda a: a.reshape(LAYERS, 1, -1)
    return dict(
        x=own(images), cot=own(cot), valid=live.astype(F32)[:, None],
        idx_col=jnp.asarray(idx)[:, :, None], idx_row=jnp.asarray(idx)[:, None, :],
        reg_col=jnp.asarray(reg)[:, :, :, None],
        reg_row=jnp.asarray(np.tile(reg, (1, 1, 4)))[:, :, None, :],
        bias=bias, ln1_gain=row(ln1_gain), ln1_bias=row(ln1_bias), qv_bias=qv_bias,
        proj_bias=row(proj_bias), ln2_gain=row(ln2_gain), ln2_bias=row(ln2_bias),
        fc1_bias=row(fc1_bias), fc2_bias=row(fc2_bias),
    )


def table_grads(ds):
    heads = 16
    entries = (2 * WIN - 1) ** 2
    entry = jnp.asarray(bias_onehot().reshape(-1))
    onehot = (entry[:, None] == jnp.arange(entries, dtype=jnp.int32)[None, :]).astype(F32)
    flat = ds.reshape(LAYERS, heads // 4, PADC, 4, PADC).transpose(0, 1, 3, 2, 4)
    return lax.dot_general(
        flat.reshape(LAYERS * heads, PADC * PADC), onehot, (((1,), (0,)), ((), ())),
        precision=lax.Precision.HIGHEST,
    ).reshape(LAYERS, heads, entries)


def pack_weights(w_qkv, w_proj, w_fc1, w_fc2):
    rows = w_qkv.shape[1]
    first = jnp.concatenate([w_qkv.reshape(LAYERS, rows, -1), w_proj.swapaxes(1, 2)], 2)
    return jnp.stack([first, w_fc1, w_fc2.swapaxes(1, 2)], 1)


def gather_plain(shard):
    full = lax.all_gather(shard, "dp", axis=2, tiled=True)
    return lax.all_gather(full, "mp", axis=2, tiled=False)


def scatter_plain(grad):
    half = lax.psum_scatter(grad, "mp", scatter_dimension=2, tiled=False)
    return lax.psum_scatter(half, "dp", scatter_dimension=2, tiled=True).astype(F32)


def per_device(
    images, loads, cotangent, ln1_gain, ln1_bias, w_qkv, qv_bias, rel_table, w_proj, proj_bias,
    ln2_gain, ln2_bias, w_fc1, fc1_bias, w_fc2, fc2_bias,
):
    mp = lax.axis_index("mp")
    n_dp = lax.axis_size("dp")
    zs = n_dp // 4
    qv_all = lax.all_gather(qv_bias, "mp", axis=2, tiled=True)
    table_all = lax.all_gather(rel_table, "mp", axis=1, tiled=True)
    fc1_all = lax.all_gather(fc1_bias, "mp", axis=1, tiled=True)
    smalls = (ln1_gain, ln1_bias, qv_all, table_all, proj_bias, ln2_gain, ln2_bias, fc1_all, fc2_bias)
    ins = small_inputs(images, cotangent, loads[0], mp, smalls)
    shard = pack_weights(w_qkv, w_proj, w_fc1, w_fc2)
    full = gather_plain(shard)
    outs = compute_call(ins, full.reshape(LAYERS, 3, 2, zs, D // zs, 1024))
    grad = scatter_plain(outs["G"].reshape(LAYERS, 3, 2, D, 1024))
    sg, tab = lax.psum((outs["SG"], table_grads(outs["DS"])), ("dp", "mp"))
    both = lax.all_gather(
        jnp.stack([outs["result"], outs["gimg"]])[:, : OWN * TOK_IMG], "mp", axis=1, tiled=True
    )
    result, gimg = both.reshape(2, 2 * OWN, TOK_IMG, D)
    rows = w_qkv.shape[1]
    q_sum = lax.dynamic_slice_in_dim(sg[:, 2, 2 * D :].reshape(LAYERS, 2, 2, HALF), mp, 1, 2)
    return (
        result,
        gimg,
        sg[:, 1, :D],
        sg[:, 1, D : 2 * D],
        grad[:, 0, :, : 3 * HALF].reshape(LAYERS, rows, 3, HALF),
        q_sum.reshape(LAYERS, 2, HALF),
        lax.dynamic_slice_in_dim(tab, mp * 8, 8, 1),
        grad[:, 0, :, 3 * HALF :].swapaxes(1, 2),
        sg[:, 2, :D],
        sg[:, 1, 2 * D : 3 * D],
        sg[:, 1, 3 * D :],
        grad[:, 1],
        lax.dynamic_slice_in_dim(sg[:, 0], mp * 1024, 1024, 1),
        grad[:, 2].swapaxes(1, 2),
        sg[:, 2, D : 2 * D],
    )


def solution(mesh):
    wq, cols = P(None, "dp", None, "mp"), P(None, "mp")
    rows_dp, cols_dp = P(None, "dp", "mp"), P(None, "mp", "dp")
    img = P("dp", None, None)
    qv, tab = P(None, None, "mp"), P(None, "mp", None)
    return jax.shard_map(
        per_device,
        mesh=mesh,
        in_specs=(
            img, P("dp"), img, P(), P(), wq, qv, tab, cols_dp, P(), P(), P(), rows_dp, cols, cols_dp, P(),
        ),
        out_specs=(img, img, P(), P(), wq, qv, tab, cols_dp, P(), P(), P(), rows_dp, cols, cols_dp, P()),
        check_vma=False,
    )
```

```python
import functools
import types

import jax
import jax.numpy as jnp
import numpy as np
from jax import lax
from jax.experimental import pallas as pl
from jax.experimental.pallas import tpu as pltpu
from jax.sharding import PartitionSpec as P

D = 512
HD = 32
FF = 2048
SIDE = 14
WIN = 7
SHIFT = 3
LAYERS = 2
TOK_IMG = SIDE * SIDE
CELLS = WIN * WIN
PADC = 64
EPS = 1e-05
MASKED = -1e30
INV_ROOT_TWO = 0.7071067811865476
INV_ROOT_TWOPI = 0.3989422804014327
SCALE_Q = HD**-0.5

OWN = 2
ROWS = 400
WROWS = OWN * 4 * PADC
STEP = 80
HALF = 256
F32 = jnp.float32
BF16 = jnp.bfloat16


def token_maps():
    idx = np.full((LAYERS, WROWS), -1, np.int32)
    reg = np.zeros((LAYERS, 4, PADC), np.int32)
    for layer in range(LAYERS):
        shift = SHIFT if layer % 2 else 0
        for win in range(OWN * 4):
            img, wr, wc = win // 4, (win // 2) % 2, win % 2
            for cell in range(CELLS):
                r, c = wr * WIN + cell // WIN, wc * WIN + cell % WIN
                idx[layer, win * PADC + cell] = (
                    img * TOK_IMG + ((r + shift) % SIDE) * SIDE + (c + shift) % SIDE
                )
                if shift:
                    band = lambda v: 0 if v < SIDE - WIN else (1 if v < SIDE - SHIFT else 2)
                    reg[layer, win % 4, cell] = 3 * band(r) + band(c)
    return idx, reg


def bias_onehot():
    cells = np.arange(CELLS)
    r, c = cells // WIN, cells % WIN
    entry = (r[None, :] - r[:, None] + WIN - 1) * (2 * WIN - 1) + (
        c[None, :] - c[:, None] + WIN - 1
    )
    full = np.full((PADC, PADC), -1, np.int32)
    full[:CELLS, :CELLS] = entry
    return full


def dot(a, b):
    return jnp.dot(a, b, preferred_element_type=F32)


def dot_nt(a, b):
    return lax.dot_general(a, b, (((1,), (1,)), ((), ())), preferred_element_type=F32)


def dot_tn(a, b):
    return lax.dot_general(a, b, (((0,), (0,)), ((), ())), preferred_element_type=F32)


def lane_head(shape):
    return lax.broadcasted_iota(jnp.int32, shape, 1) // HD


def spread_heads(block):
    head = lane_head(block.shape)
    zero = jnp.zeros_like(block)
    return jnp.concatenate([jnp.where(head == h, block, zero) for h in range(4)], axis=0)


def gather_heads(stack):
    head = lane_head((PADC, 128))
    total = jnp.where(head == 0, stack[:PADC], 0.0)
    for h in range(1, 4):
        total = total + jnp.where(head == h, stack[h * PADC : (h + 1) * PADC], 0.0)
    return total


def row_loop(body, init):
    def step(i, carry):
        return body(pl.ds(pl.multiple_of(i * STEP, STEP), STEP), carry)

    return lax.fori_loop(0, ROWS // STEP, step, init)


def weight(r, l, g, x, cols):
    part = r.W[l, g, x, :, :, :, :, cols]
    return part.reshape(D, part.shape[-1])


def weight_rows(r, l, g, x, n, cols):
    per = r.W.shape[3] // 2
    part = r.W[l, g, x, pl.ds(n * per, per), :, :, :, cols]
    return part.reshape(HALF, part.shape[-1])


def put_grad(r, l, g, x, cols, value):
    lead = r.G.shape[3:7]
    r.G[l, g, x, :, :, :, :, cols] = value.astype(BF16).reshape(lead + value.shape[-1:])


def norm_into(r, l, src, normed, rstd_ref, gain, shift, out):
    def body(rows, carry):
        s = src[rows, :]
        centre = s - jnp.mean(s, -1, keepdims=True)
        rstd = lax.rsqrt(jnp.mean(centre * centre, -1, keepdims=True) + EPS)
        n = centre * rstd
        normed[l, rows, :] = n
        rstd_ref[l, rows, :] = rstd
        out[rows, :] = (n * gain[l] + shift[l]).astype(BF16)
        return carry

    row_loop(body, 0)


def norm_back(r, l, grad_y, normed, rstd_ref, gain, base, out, out_low):
    def body(rows, carry):
        gain_sum, shift_sum, out_sum = carry
        gy = grad_y[rows, :]
        n = normed[l, rows, :]
        e = gy * gain[l]
        back = rstd_ref[l, rows, :] * (
            e - jnp.mean(e, -1, keepdims=True) - n * jnp.mean(e * n, -1, keepdims=True)
        )
        res = base[rows, :] + back
        out[rows, :] = res
        out_low[rows, :] = res.astype(BF16)
        return (
            gain_sum + jnp.sum(gy * n, 0, keepdims=True),
            shift_sum + jnp.sum(gy, 0, keepdims=True),
            out_sum + jnp.sum(res, 0, keepdims=True),
        )

    zero = jnp.zeros((1, D), F32)
    return row_loop(body, (zero, zero, zero))


def to_windows(r, l):
    tok = lax.broadcasted_iota(jnp.int32, (WROWS, ROWS), 1)
    return jnp.where(tok == r.idx_col[l], 1.0, 0.0).astype(BF16)


def to_grid(r, l):
    tok = lax.broadcasted_iota(jnp.int32, (ROWS, WROWS), 0)
    return jnp.where(tok == r.idx_row[l], 1.0, 0.0).astype(BF16)


def attention_forward(r, l):
    def window(w, carry):
        rows = pl.ds(pl.multiple_of(w * PADC, PADC), PADC)
        pos = lax.rem(w, 4)
        same = r.reg_col[l, pos] == r.reg_row[l, pos]
        for g in range(4):
            lanes = slice(g * 128, (g + 1) * 128)
            q, k, v = r.Q[l, rows, lanes], r.K[l, rows, lanes], r.V[l, rows, lanes]
            s = dot_nt(k, spread_heads(q)) + r.bias[l, g]
            s = jnp.where(same, s, MASKED)
            e = jnp.exp(s - jnp.max(s, 0, keepdims=True))
            p = (e / jnp.sum(e, 0, keepdims=True)).astype(BF16)
            r.PR[l, w * 4 + g] = p
            r.AW[rows, lanes] = gather_heads(dot_tn(p, v)).astype(BF16)
        return carry

    lax.fori_loop(0, OWN * 4, window, 0)


def attention_backward(r, l):
    zero = jnp.zeros((1, 128), F32)

    def window(w, carry):
        rows = pl.ds(pl.multiple_of(w * PADC, PADC), PADC)
        sums = list(carry)
        for g in range(4):
            lanes = slice(g * 128, (g + 1) * 128)
            q, k, v = r.Q[l, rows, lanes], r.K[l, rows, lanes], r.V[l, rows, lanes]
            da = r.AW[rows, lanes]
            p = r.PR[l, w * 4 + g]
            da_spread = spread_heads(da)
            pf = p.astype(F32)
            pg = dot_nt(v, da_spread)
            ds = pf * (pg - jnp.sum(pf * pg, 0, keepdims=True))
            r.DS[l, g] += ds
            low = ds.astype(BF16)
            dv = dot(p, da_spread)
            dk = dot(low, spread_heads(q))
            dq = gather_heads(dot_tn(low, k)) * SCALE_Q
            x, at = g // 2, (g % 2) * 128
            r.DM[x, rows, at : at + 128] = dq.astype(BF16)
            r.DM[x, rows, HALF + at : HALF + at + 128] = dk.astype(BF16)
            r.DM[x, rows, 2 * HALF + at : 2 * HALF + at + 128] = dv.astype(BF16)
            sums[g] = sums[g] + jnp.sum(dq, 0, keepdims=True)
            sums[4 + g] = sums[4 + g] + jnp.sum(dv, 0, keepdims=True)
        return tuple(sums)

    return lax.fori_loop(0, OWN * 4, window, (zero,) * 8)


def forward(r, l):
    norm_into(r, l, r.S, r.N1, r.R1, r.ln1_gain, r.ln1_bias, r.YB)
    r.YW[l] = dot(to_windows(r, l), r.YB[...]).astype(BF16)
    yw = r.YW[l]
    for x in range(2):
        cols = slice(x * HALF, (x + 1) * HALF)
        q = dot(yw, weight(r, l, 0, x, slice(0, HALF)))
        r.Q[l, :, cols] = ((q + r.qv_bias[l, 0:1, cols]) * SCALE_Q).astype(BF16)
        r.K[l, :, cols] = dot(yw, weight(r, l, 0, x, slice(HALF, 2 * HALF))).astype(BF16)
        v = dot(yw, weight(r, l, 0, x, slice(2 * HALF, 3 * HALF)))
        r.V[l, :, cols] = (v + r.qv_bias[l, 1:2, cols]).astype(BF16)
    attention_forward(r, l)
    r.AT[l] = dot(to_grid(r, l), r.AW[...]).astype(BF16)
    for n in range(2):
        cols = slice(n * HALF, (n + 1) * HALF)
        acc = dot_nt(r.AT[l, :, :HALF], weight_rows(r, l, 0, 0, n, slice(3 * HALF, 4 * HALF)))
        acc += dot_nt(r.AT[l, :, HALF:], weight_rows(r, l, 0, 1, n, slice(3 * HALF, 4 * HALF)))
        r.S[:, cols] = r.S[:, cols] + acc + r.proj_bias[l, :, cols]
    norm_into(r, l, r.S, r.N2, r.R2, r.ln2_gain, r.ln2_bias, r.YB)
    r.Y2[l] = r.YB[...]
    for x in range(2):

        def up(n, carry):
            at = pl.ds(pl.multiple_of(n * HALF, HALF), HALF)
            full = pl.ds(pl.multiple_of(x * 1024 + n * HALF, HALF), HALF)
            pre = dot(r.YB[...], weight(r, l, 1, x, at)) + r.fc1_bias[l, :, full]
            phi = 0.5 * (1.0 + lax.erf(pre * INV_ROOT_TWO))
            r.AC[l, :, full] = (pre * phi).astype(BF16)
            dens = jnp.exp(-0.5 * pre * pre) * INV_ROOT_TWOPI
            r.SL[l, :, full] = (phi + pre * dens).astype(BF16)
            return carry

        lax.fori_loop(0, 4, up, 0)
    for n in range(2):
        cols = slice(n * HALF, (n + 1) * HALF)
        acc = dot_nt(r.AC[l, :, :1024], weight_rows(r, l, 2, 0, n, slice(0, 1024)))
        acc += dot_nt(r.AC[l, :, 1024:], weight_rows(r, l, 2, 1, n, slice(0, 1024)))
        r.S[:, cols] = r.S[:, cols] + acc + r.fc2_bias[l, :, cols]


def backward_mlp(r, l):
    def low(rows, total):
        g = r.S[rows, :]
        r.YB[rows, :] = g.astype(BF16)
        return total + jnp.sum(g, 0, keepdims=True)

    r.SG[l, 2:3, D : 2 * D] = row_loop(low, jnp.zeros((1, D), F32))
    r.TA[...] = r.YB[...].T
    r.TB[...] = r.Y2[l].T
    for x in range(2):

        def down(n, carry):
            at = pl.ds(pl.multiple_of(n * HALF, HALF), HALF)
            full = pl.ds(pl.multiple_of(x * 1024 + n * HALF, HALF), HALF)
            pg = dot(r.YB[...], weight(r, l, 2, x, at)) * r.SL[l, :, full].astype(F32)
            r.SG[l, 0:1, full] = jnp.sum(pg, 0, keepdims=True)
            pb = pg.astype(BF16)
            r.PB[:, full] = pb
            put_grad(r, l, 2, x, at, dot(r.TA[...], r.AC[l, :, full]))
            put_grad(r, l, 1, x, at, dot(r.TB[...], pb))
            return carry

        lax.fori_loop(0, 4, down, 0)
    for n in range(2):
        cols = slice(n * HALF, (n + 1) * HALF)
        acc = dot_nt(r.PB[:, :1024], weight_rows(r, l, 1, 0, n, slice(0, 1024)))
        acc += dot_nt(r.PB[:, 1024:], weight_rows(r, l, 1, 1, n, slice(0, 1024)))
        r.GY[:, cols] = acc
    gain, shift, out = norm_back(r, l, r.GY, r.N2, r.R2, r.ln2_gain, r.S, r.S, r.YB)
    r.SG[l, 1:2, 2 * D : 3 * D] = gain
    r.SG[l, 1:2, 3 * D :] = shift
    r.SG[l, 2:3, :D] = out


def backward_attention(r, l):
    r.TA[...] = r.YB[...].T
    for x in range(2):
        cols = slice(x * HALF, (x + 1) * HALF)
        put_grad(r, l, 0, x, slice(3 * HALF, 4 * HALF), dot(r.TA[...], r.AT[l, :, cols]))
        att = dot(r.YB[...], weight(r, l, 0, x, slice(3 * HALF, 4 * HALF)))
        r.GB[:, cols] = att.astype(BF16)
    r.AW[...] = dot(to_windows(r, l), r.GB[...]).astype(BF16)
    r.DS[l] = jnp.zeros_like(r.DS[l])
    sums = attention_backward(r, l)
    for g in range(4):
        r.SG[l, 2:3, 2 * D + g * 128 : 2 * D + (g + 1) * 128] = sums[g]
        r.SG[l, 2:3, 3 * D + g * 128 : 3 * D + (g + 1) * 128] = sums[4 + g]
    r.TW[...] = r.YW[l].T
    for x in range(2):
        for part in range(3):
            cols = slice(part * HALF, (part + 1) * HALF)
            put_grad(r, l, 0, x, cols, dot(r.TW[...], r.DM[x, :, cols]))
    for n in range(2):
        cols = slice(n * HALF, (n + 1) * HALF)
        acc = dot_nt(r.DM[0], weight_rows(r, l, 0, 0, n, slice(0, 3 * HALF)))
        acc += dot_nt(r.DM[1], weight_rows(r, l, 0, 1, n, slice(0, 3 * HALF)))
        r.AW[:, cols] = acc.astype(BF16)
    r.GY[...] = dot(to_grid(r, l), r.AW[...])
    gain, shift, _ = norm_back(r, l, r.GY, r.N1, r.R1, r.ln1_gain, r.S, r.S, r.YB)
    r.SG[l, 1:2, :D] = gain
    r.SG[l, 1:2, D : 2 * D] = shift


INPUTS = (
    "x", "cot", "valid", "idx_col", "idx_row", "reg_col", "reg_row", "bias",
    "ln1_gain", "ln1_bias", "qv_bias", "proj_bias", "ln2_gain", "ln2_bias", "fc1_bias", "fc2_bias",
)
SMALL_ROWS = 8


def scratch_spec():
    return dict(
        S=pltpu.VMEM((ROWS, D), F32),
        GY=pltpu.VMEM((ROWS, D), F32),
        YB=pltpu.VMEM((ROWS, D), BF16),
        GB=pltpu.VMEM((ROWS, D), BF16),
        N1=pltpu.VMEM((LAYERS, ROWS, D), F32),
        N2=pltpu.VMEM((LAYERS, ROWS, D), F32),
        R1=pltpu.VMEM((LAYERS, ROWS, 1), F32),
        R2=pltpu.VMEM((LAYERS, ROWS, 1), F32),
        YW=pltpu.VMEM((LAYERS, WROWS, D), BF16),
        Q=pltpu.VMEM((LAYERS, WROWS, D), BF16),
        K=pltpu.VMEM((LAYERS, WROWS, D), BF16),
        V=pltpu.VMEM((LAYERS, WROWS, D), BF16),
        PR=pltpu.VMEM((LAYERS, OWN * 16, PADC, 4 * PADC), BF16),
        AW=pltpu.VMEM((WROWS, D), BF16),
        AT=pltpu.VMEM((LAYERS, ROWS, D), BF16),
        Y2=pltpu.VMEM((LAYERS, ROWS, D), BF16),
        AC=pltpu.VMEM((LAYERS, ROWS, FF), BF16),
        SL=pltpu.VMEM((LAYERS, ROWS, FF), BF16),
        PB=pltpu.VMEM((ROWS, FF), BF16),
        DM=pltpu.VMEM((2, WROWS, 3 * HALF), BF16),
        TA=pltpu.VMEM((D, ROWS), BF16),
        TB=pltpu.VMEM((D, ROWS), BF16),
        TW=pltpu.VMEM((D, WROWS), BF16),
    )


def compute_kernel(names, *refs):
    r = types.SimpleNamespace(**dict(zip(names, refs)))
    r.S[...] = r.x[...].astype(F32)
    lax.fori_loop(0, LAYERS, lambda l, c: (forward(r, l), c)[1], 0)
    r.result[...] = (r.S[...] * r.valid[...]).astype(BF16)
    r.S[...] = r.cot[...].astype(F32) * r.valid[...]

    def back(i, c):
        l = LAYERS - 1 - i
        backward_mlp(r, l)
        backward_attention(r, l)
        return c

    lax.fori_loop(0, LAYERS, back, 0)
    r.gimg[...] = r.YB[...]


def compute_call(ins, w):
    outs = dict(
        G=jax.ShapeDtypeStruct(w.shape, BF16),
        SG=jax.ShapeDtypeStruct((LAYERS, SMALL_ROWS, FF), F32),
        DS=jax.ShapeDtypeStruct((LAYERS, 4, PADC, 4 * PADC), F32),
        result=jax.ShapeDtypeStruct((ROWS, D), BF16),
        gimg=jax.ShapeDtypeStruct((ROWS, D), BF16),
    )
    scratch = scratch_spec()
    names = INPUTS + ("W",) + tuple(outs) + tuple(scratch)
    got = pl.pallas_call(
        functools.partial(compute_kernel, names),
        out_shape=list(outs.values()),
        in_specs=[pl.BlockSpec(memory_space=pltpu.VMEM)] * (len(INPUTS) + 1),
        out_specs=[pl.BlockSpec(memory_space=pltpu.VMEM)] * len(outs),
        scratch_shapes=list(scratch.values()),
        compiler_params=pltpu.CompilerParams(vmem_limit_bytes=67043328),
        name="step",
    )(*[ins[name] for name in INPUTS], w)
    return dict(zip(outs, got))


def small_inputs(images, cot, load, mp, smalls):
    idx, reg = token_maps()
    keep = OWN * TOK_IMG

    def own(arr):
        rows = lax.dynamic_slice_in_dim(arr.reshape(-1, D), mp * keep, keep, 0)
        return jnp.pad(rows, ((0, ROWS - keep), (0, 0)))

    slot = mp * OWN + jnp.arange(ROWS, dtype=jnp.int32) // TOK_IMG
    live = (slot < load) & (jnp.arange(ROWS) < keep)
    ln1_gain, ln1_bias, qv_bias, rel_table, proj_bias, ln2_gain, ln2_bias, fc1_bias, fc2_bias = smalls
    heads = rel_table.shape[1]
    entries = rel_table.shape[2]
    entry = jnp.asarray(bias_onehot().reshape(-1))
    onehot = (entry[:, None] == jnp.arange(entries, dtype=jnp.int32)[None, :]).astype(F32)
    flat = lax.dot_general(
        onehot, rel_table.reshape(LAYERS * heads, entries), (((1,), (1,)), ((), ())),
        precision=lax.Precision.HIGHEST,
    )
    bias = flat.reshape(PADC, PADC, LAYERS, heads // 4, 4).transpose(2, 3, 0, 4, 1)
    pad_key = jnp.arange(PADC)[:, None, None] >= CELLS
    bias = jnp.where(pad_key, MASKED, bias).reshape(LAYERS, heads // 4, PADC, 4 * PADC)
    row = lambda a: a.reshape(LAYERS, 1, -1)
    return dict(
        x=own(images), cot=own(cot), valid=live.astype(F32)[:, None],
        idx_col=jnp.asarray(idx)[:, :, None], idx_row=jnp.asarray(idx)[:, None, :],
        reg_col=jnp.asarray(reg)[:, :, :, None],
        reg_row=jnp.asarray(np.tile(reg, (1, 1, 4)))[:, :, None, :],
        bias=bias, ln1_gain=row(ln1_gain), ln1_bias=row(ln1_bias), qv_bias=qv_bias,
        proj_bias=row(proj_bias), ln2_gain=row(ln2_gain), ln2_bias=row(ln2_bias),
        fc1_bias=row(fc1_bias), fc2_bias=row(fc2_bias),
    )


def table_grads(ds):
    heads = 16
    entries = (2 * WIN - 1) ** 2
    entry = jnp.asarray(bias_onehot().reshape(-1))
    onehot = (entry[:, None] == jnp.arange(entries, dtype=jnp.int32)[None, :]).astype(F32)
    flat = ds.reshape(LAYERS, heads // 4, PADC, 4, PADC).transpose(0, 1, 3, 2, 4)
    return lax.dot_general(
        flat.reshape(LAYERS * heads, PADC * PADC), onehot, (((1,), (0,)), ((), ())),
        precision=lax.Precision.HIGHEST,
    ).reshape(LAYERS, heads, entries)


def pack_weights(w_qkv, w_proj, w_fc1, w_fc2):
    rows = w_qkv.shape[1]
    first = jnp.concatenate([w_qkv.reshape(LAYERS, rows, -1), w_proj.swapaxes(1, 2)], 2)
    return jnp.stack([first, w_fc1, w_fc2.swapaxes(1, 2)], 1)


MESH = pl.DeviceIdType.MESH
UNITS = 3 * LAYERS
Z_SIDE = 4


class Place:
    def __init__(self):
        self.dp = lax.axis_index("dp")
        self.x = lax.axis_index("mp")
        self.c = lax.rem(self.dp, 2)
        self.y = lax.rem(self.dp // 2, 2)
        self.z = self.dp // 4
        self.sib = {"dp": self.dp + 1 - 2 * self.c, "mp": self.x}
        self.ynbr = {"dp": self.dp + 2 - 4 * self.y, "mp": self.x}
        self.xnbr = {"dp": self.dp, "mp": 1 - self.x}

    def zpos(self, k):
        return lax.rem(self.z + k, Z_SIDE)

    def zpeer(self, k):
        return {"dp": self.zpos(k) * 4 + lax.rem(self.dp, 4), "mp": self.x}

    def peers(self):
        return [self.sib, self.ynbr, self.xnbr] + [self.zpeer(k) for k in range(1, Z_SIDE)]


def greet(place):
    barrier = pltpu.get_barrier_semaphore()
    peers = place.peers()
    for peer in peers:
        pl.semaphore_signal(barrier, inc=1, device_id=peer, device_id_type=MESH)
    pl.semaphore_wait(barrier, len(peers))


def remote(src, dst, sems, u, k, peer):
    return pltpu.make_async_remote_copy(
        src_ref=src, dst_ref=dst, send_sem=sems.at[0, u, k], recv_sem=sems.at[1, u, k],
        device_id=peer, device_id_type=MESH,
    )


def landed(dst, sems, u, k, peer):
    remote(dst, dst, sems, u, k, peer).wait_recv()


TOP, LOW = pl.ds(0, 16), pl.ds(16, 16)


class Gather:
    def __init__(self, place, shard, w, sems, local):
        self.p, self.shard, self.w, self.sems, self.local = place, shard, w, sems, local

    def slab(self, u, x, y, c, part=None):
        ref = self.w.at[u // 3, lax.rem(u, 3), x, :, y, c]
        return ref if part is None else ref.at[:, part]

    def block(self, u, z):
        p = self.p
        return self.w.at[u // 3, lax.rem(u, 3), p.x, z, p.y, p.c]

    def own(self, u):
        return self.shard.at[u // 3, lax.rem(u, 3)]

    def z_copy(self, u, k):
        return remote(self.own(u), self.block(u, self.p.z), self.sems, u, k - 1, self.p.zpeer(k))

    def local_copy(self, u):
        return pltpu.make_async_copy(self.own(u), self.block(u, self.p.z), self.local.at[u])

    def full_copies(self, u):
        p = self.p
        mine = self.slab(u, p.x, p.y, p.c)
        return [
            remote(mine, mine, self.sems, u, 3, p.xnbr),
            remote(mine, mine, self.sems, u, 4, p.ynbr),
            remote(mine, mine, self.sems, u, 5, p.sib),
        ]

    def half_copies(self, u):
        p = self.p
        from_y, from_x = (p.x, 1 - p.y, p.c), (1 - p.x, p.y, p.c)
        top, low = self.slab(u, *from_y, TOP), self.slab(u, *from_x, LOW)
        fy, fx = self.slab(u, *from_y), self.slab(u, *from_x)
        return [
            remote(top, top, self.sems, u, 6, p.xnbr),
            remote(low, low, self.sems, u, 7, p.ynbr),
            remote(fx, fx, self.sems, u, 8, p.sib),
            remote(fy, fy, self.sems, u, 9, p.sib),
        ]

    def last_copies(self, u):
        p = self.p
        far = self.slab(u, 1 - p.x, 1 - p.y, p.c)
        return [remote(far, far, self.sems, u, 10, p.sib)]

    def start_own(self, u):
        self.local_copy(u).start()
        for k in range(1, Z_SIDE):
            self.z_copy(u, k).start()

    def pass_own(self, u):
        p = self.p
        self.local_copy(u).wait()
        for k in range(1, Z_SIDE):
            landed(self.block(u, p.zpos(Z_SIDE - k)), self.sems, u, k - 1, p.zpeer(Z_SIDE - k))
        for copy in self.full_copies(u):
            copy.start()

    def pass_near(self, u):
        p = self.p
        landed(self.slab(u, 1 - p.x, p.y, p.c), self.sems, u, 3, p.xnbr)
        landed(self.slab(u, p.x, 1 - p.y, p.c), self.sems, u, 4, p.ynbr)
        for copy in self.half_copies(u):
            copy.start()

    def pass_far(self, u):
        p = self.p
        landed(self.slab(u, 1 - p.x, 1 - p.y, p.c, TOP), self.sems, u, 6, p.xnbr)
        landed(self.slab(u, 1 - p.x, 1 - p.y, p.c, LOW), self.sems, u, 7, p.ynbr)
        for copy in self.last_copies(u):
            copy.start()

    def ready(self, u):
        p = self.p
        for k, (x, y) in ((5, (p.x, p.y)), (8, (1 - p.x, p.y)), (9, (p.x, 1 - p.y)), (10, (1 - p.x, 1 - p.y))):
            landed(self.slab(u, x, y, 1 - p.c), self.sems, u, k, p.sib)

    def tick(self, t):
        @pl.when(t < UNITS)
        def _():
            self.pass_own(t)

        @pl.when(t + 2 < UNITS)
        def _():
            self.start_own(t + 2)

        @pl.when((t >= 1) & (t - 1 < UNITS))
        def _():
            self.pass_near(t - 1)

        @pl.when((t >= 2) & (t - 2 < UNITS))
        def _():
            self.pass_far(t - 2)

    def drain(self, u):
        for k in range(1, Z_SIDE):
            self.z_copy(u, k).wait_send()
        for copy in self.full_copies(u) + self.half_copies(u) + self.last_copies(u):
            copy.wait_send()


def gather_kernel(shard, w, sems, local):
    place = Place()
    greet(place)
    gather = Gather(place, shard, w, sems, local)
    gather.start_own(0)
    gather.start_own(1)

    def tick(t, c):
        gather.tick(t)
        return c

    lax.fori_loop(0, UNITS + 2, tick, 0)

    def finish(u, c):
        gather.ready(u)
        gather.drain(u)
        return c

    lax.fori_loop(0, UNITS, finish, 0)


def gather_call(shard):
    return pl.pallas_call(
        gather_kernel,
        out_shape=jax.ShapeDtypeStruct((LAYERS, 3, 2, Z_SIDE, 2, 2, 32, 1024), BF16),
        in_specs=[pl.BlockSpec(memory_space=pltpu.VMEM)],
        out_specs=pl.BlockSpec(memory_space=pltpu.VMEM),
        scratch_shapes=[pltpu.SemaphoreType.DMA((2, UNITS, 11)), pltpu.SemaphoreType.DMA((UNITS,))],
        compiler_params=pltpu.CompilerParams(
            collective_id=0, has_side_effects=True, vmem_limit_bytes=40 << 20
        ),
        name="gather",
    )(shard)


class Scatter:
    def __init__(self, place, r):
        self.p, self.r, self.sems = place, r, r.sums

    def at(self, ref, u):
        return ref.at[u // 3, lax.rem(u, 3)]

    def sib_copy(self, u):
        p, r = self.p, self.r
        return remote(
            self.at(r.G, u).at[:, :, :, 1 - p.c], self.at(r.P, u), self.sems, u, 0, p.sib
        )

    def part(self, u, x, y, rows=None):
        ref = self.at(self.r.P, u).at[x, :, y]
        return ref if rows is None else ref.at[:, rows]

    def far_copies(self, u):
        p, r = self.p, self.r
        return [
            remote(self.part(u, 1 - p.x, 1 - p.y, TOP), self.at(r.RA, u).at[0], self.sems, u, 1, p.xnbr),
            remote(self.part(u, 1 - p.x, 1 - p.y, LOW), self.at(r.RA, u).at[1], self.sems, u, 2, p.ynbr),
        ]

    def near_copies(self, u):
        p, r = self.p, self.r
        return [
            remote(self.part(u, 1 - p.x, p.y), self.at(r.RB, u).at[0], self.sems, u, 3, p.xnbr),
            remote(self.part(u, p.x, 1 - p.y), self.at(r.RB, u).at[1], self.sems, u, 4, p.ynbr),
        ]

    def z_copy(self, u, k):
        p, r = self.p, self.r
        src = self.at(r.P, u).at[p.x, p.zpos(k), p.y]
        return remote(src, self.at(r.RC, u).at[k - 1], self.sems, u, 4 + k, p.zpeer(k))

    def start_sib(self, u):
        self.sib_copy(u).start()

    def add(self, dst, *srcs):
        for z in range(Z_SIDE):
            total = dst[z].astype(F32)
            for src in srcs:
                total = total + src[z].astype(F32)
            dst[z] = total.astype(BF16)

    def start_far(self, u):
        p, r = self.p, self.r
        landed(self.at(r.P, u), self.sems, u, 0, p.sib)
        grads = self.at(r.G, u)
        self.add(self.part(u, 1 - p.x, 1 - p.y), grads.at[1 - p.x, :, 1 - p.y, p.c])
        for copy in self.far_copies(u):
            copy.start()
        for x, y in ((1 - p.x, p.y), (p.x, 1 - p.y), (p.x, p.y)):
            self.add(self.part(u, x, y), grads.at[x, :, y, p.c])

    def start_near(self, u):
        p, r = self.p, self.r
        landed(self.at(r.RA, u).at[0], self.sems, u, 1, p.xnbr)
        landed(self.at(r.RA, u).at[1], self.sems, u, 2, p.ynbr)
        self.add(self.part(u, p.x, 1 - p.y, TOP), self.at(r.RA, u).at[0])
        self.add(self.part(u, 1 - p.x, p.y, LOW), self.at(r.RA, u).at[1])
        for copy in self.near_copies(u):
            copy.start()

    def start_z(self, u):
        p, r = self.p, self.r
        landed(self.at(r.RB, u).at[0], self.sems, u, 3, p.xnbr)
        landed(self.at(r.RB, u).at[1], self.sems, u, 4, p.ynbr)
        self.add(self.part(u, p.x, p.y), self.at(r.RB, u).at[0], self.at(r.RB, u).at[1])
        for k in range(1, Z_SIDE):
            self.z_copy(u, k).start()

    def finish(self, u):
        p, r = self.p, self.r
        total = r.P[u // 3, lax.rem(u, 3), p.x, p.z, p.y].astype(F32)
        for k in range(1, Z_SIDE):
            landed(self.at(r.RC, u).at[k - 1], self.sems, u, 4 + k, p.zpeer(Z_SIDE - k))
            total = total + r.RC[u // 3, lax.rem(u, 3), k - 1].astype(F32)
        r.grad[u // 3, lax.rem(u, 3)] = total

    def drain(self, u):
        for copy in [self.sib_copy(u)] + self.far_copies(u) + self.near_copies(u):
            copy.wait_send()
        for k in range(1, Z_SIDE):
            self.z_copy(u, k).wait_send()


def scatter_scratch():
    lead = (LAYERS, 3)
    return dict(
        P=pltpu.VMEM(lead + (2, Z_SIDE, 2, 32, 1024), BF16),
        RA=pltpu.VMEM(lead + (2, Z_SIDE, 16, 1024), BF16),
        RB=pltpu.VMEM(lead + (2, Z_SIDE, 32, 1024), BF16),
        RC=pltpu.VMEM(lead + (3, 32, 1024), BF16),
        sums=pltpu.SemaphoreType.DMA((2, UNITS, 8)),
    )


def scatter_kernel(names, *refs):
    r = types.SimpleNamespace(**dict(zip(names, refs)))
    place = Place()
    greet(place)
    scatter = Scatter(place, r)

    def tick(t, c):
        for lag, stage in enumerate(
            (scatter.start_sib, scatter.start_far, scatter.start_near, scatter.start_z, scatter.finish)
        ):
            u = t - lag

            @pl.when((u >= 0) & (u < UNITS))
            def _():
                stage(u)

        return c

    lax.fori_loop(0, UNITS + 4, tick, 0)

    def finish(u, c):
        scatter.drain(u)
        return c

    lax.fori_loop(0, UNITS, finish, 0)


def scatter_call(g):
    scratch = scatter_scratch()
    names = ("G", "grad") + tuple(scratch)
    return pl.pallas_call(
        functools.partial(scatter_kernel, names),
        out_shape=jax.ShapeDtypeStruct((LAYERS, 3, 32, 1024), F32),
        in_specs=[pl.BlockSpec(memory_space=pltpu.VMEM)],
        out_specs=pl.BlockSpec(memory_space=pltpu.VMEM),
        scratch_shapes=list(scratch.values()),
        compiler_params=pltpu.CompilerParams(
            collective_id=1, has_side_effects=True, vmem_limit_bytes=48 << 20
        ),
        name="scatter",
    )(g)


def gather_plain(shard):
    full = lax.all_gather(shard, "dp", axis=2, tiled=True)
    return lax.all_gather(full, "mp", axis=2, tiled=False)


def scatter_plain(grad):
    half = lax.psum_scatter(grad, "mp", scatter_dimension=2, tiled=False)
    return lax.psum_scatter(half, "dp", scatter_dimension=2, tiled=True).astype(F32)


def per_device(
    images, loads, cotangent, ln1_gain, ln1_bias, w_qkv, qv_bias, rel_table, w_proj, proj_bias,
    ln2_gain, ln2_bias, w_fc1, fc1_bias, w_fc2, fc2_bias,
):
    mp = lax.axis_index("mp")
    n_dp = lax.axis_size("dp")
    qv_all = lax.all_gather(qv_bias, "mp", axis=2, tiled=True)
    table_all = lax.all_gather(rel_table, "mp", axis=1, tiled=True)
    fc1_all = lax.all_gather(fc1_bias, "mp", axis=1, tiled=True)
    smalls = (ln1_gain, ln1_bias, qv_all, table_all, proj_bias, ln2_gain, ln2_bias, fc1_all, fc2_bias)
    ins = small_inputs(images, cotangent, loads[0], mp, smalls)
    shard = pack_weights(w_qkv, w_proj, w_fc1, w_fc2)
    direct = n_dp == 4 * Z_SIDE and lax.axis_size("mp") == 2
    if direct:
        full = gather_call(shard)
    else:
        full = gather_plain(shard).reshape(LAYERS, 3, 2, 4, 1, 1, D // 4, 1024)
    outs = compute_call(ins, full)
    if direct:
        grad = scatter_call(outs["G"])
    else:
        grad = scatter_plain(outs["G"].reshape(LAYERS, 3, 2, D, 1024))
    sg, tab = lax.psum((outs["SG"], table_grads(outs["DS"])), ("dp", "mp"))
    both = lax.all_gather(
        jnp.stack([outs["result"], outs["gimg"]])[:, : OWN * TOK_IMG], "mp", axis=1, tiled=True
    )
    result, gimg = both.reshape(2, 2 * OWN, TOK_IMG, D)
    rows = w_qkv.shape[1]
    q_sum = lax.dynamic_slice_in_dim(sg[:, 2, 2 * D :].reshape(LAYERS, 2, 2, HALF), mp, 1, 2)
    return (
        result,
        gimg,
        sg[:, 1, :D],
        sg[:, 1, D : 2 * D],
        grad[:, 0, :, : 3 * HALF].reshape(LAYERS, rows, 3, HALF),
        q_sum.reshape(LAYERS, 2, HALF),
        lax.dynamic_slice_in_dim(tab, mp * 8, 8, 1),
        grad[:, 0, :, 3 * HALF :].swapaxes(1, 2),
        sg[:, 2, :D],
        sg[:, 1, 2 * D : 3 * D],
        sg[:, 1, 3 * D :],
        grad[:, 1],
        lax.dynamic_slice_in_dim(sg[:, 0], mp * 1024, 1024, 1),
        grad[:, 2].swapaxes(1, 2),
        sg[:, 2, D : 2 * D],
    )


def solution(mesh):
    wq, cols = P(None, "dp", None, "mp"), P(None, "mp")
    rows_dp, cols_dp = P(None, "dp", "mp"), P(None, "mp", "dp")
    img = P("dp", None, None)
    qv, tab = P(None, None, "mp"), P(None, "mp", None)
    return jax.shard_map(
        per_device,
        mesh=mesh,
        in_specs=(
            img, P("dp"), img, P(), P(), wq, qv, tab, cols_dp, P(), P(), P(), rows_dp, cols, cols_dp, P(),
        ),
        out_specs=(img, img, P(), P(), wq, qv, tab, cols_dp, P(), P(), P(), rows_dp, cols, cols_dp, P()),
        check_vma=False,
    )
```

```python
import functools
import types

import jax
import jax.numpy as jnp
import numpy as np
from jax import lax
from jax.experimental import pallas as pl
from jax.experimental.pallas import tpu as pltpu
from jax.sharding import PartitionSpec as P

D = 512
HD = 32
FF = 2048
SIDE = 14
WIN = 7
SHIFT = 3
LAYERS = 2
TOK_IMG = SIDE * SIDE
CELLS = WIN * WIN
PADC = 64
EPS = 1e-05
MASKED = -1e30
INV_ROOT_TWO = 0.7071067811865476
INV_ROOT_TWOPI = 0.3989422804014327
SCALE_Q = HD**-0.5

OWN = 2
ROWS = 400
WROWS = OWN * 4 * PADC
STEP = 80
HALF = 256
F32 = jnp.float32
BF16 = jnp.bfloat16


def token_maps():
    idx = np.full((LAYERS, WROWS), -1, np.int32)
    reg = np.zeros((LAYERS, 4, PADC), np.int32)
    for layer in range(LAYERS):
        shift = SHIFT if layer % 2 else 0
        for win in range(OWN * 4):
            img, wr, wc = win // 4, (win // 2) % 2, win % 2
            for cell in range(CELLS):
                r, c = wr * WIN + cell // WIN, wc * WIN + cell % WIN
                token = ((r + shift) % SIDE) * SIDE + (c + shift) % SIDE
                idx[layer, win * PADC + cell] = token * OWN + img
                if shift:
                    band = lambda v: 0 if v < SIDE - WIN else (1 if v < SIDE - SHIFT else 2)
                    reg[layer, win % 4, cell] = 3 * band(r) + band(c)
    return idx, reg


def dot(a, b):
    return jnp.dot(a, b, preferred_element_type=F32)


def dot_nt(a, b):
    return lax.dot_general(a, b, (((1,), (1,)), ((), ())), preferred_element_type=F32)


def dot_tn(a, b):
    return lax.dot_general(a, b, (((0,), (0,)), ((), ())), preferred_element_type=F32)


def lane_head(shape):
    return lax.broadcasted_iota(jnp.int32, shape, 1) // HD


def spread_heads(block):
    head = lane_head(block.shape)
    zero = jnp.zeros_like(block)
    return jnp.concatenate([jnp.where(head == h, block, zero) for h in range(4)], axis=0)


def gather_heads(stack):
    head = lane_head((PADC, 128))
    total = jnp.where(head == 0, stack[:PADC], 0.0)
    for h in range(1, 4):
        total = total + jnp.where(head == h, stack[h * PADC : (h + 1) * PADC], 0.0)
    return total


def row_loop(body, init):
    def step(i, carry):
        return body(pl.ds(pl.multiple_of(i * STEP, STEP), STEP), carry)

    return lax.fori_loop(0, ROWS // STEP, step, init)


def weight(r, l, g, x, cols):
    part = r.W[l, g, x, :, :, :, :, cols]
    return part.reshape(D, part.shape[-1])


def weight_rows(r, l, g, x, n, cols):
    per = r.W.shape[3] // 2
    part = r.W[l, g, x, pl.ds(n * per, per), :, :, :, cols]
    return part.reshape(HALF, part.shape[-1])


def put_grad(r, l, g, x, cols, value):
    lead = r.G.shape[3:7]
    r.G[l, g, x, :, :, :, :, cols] = value.astype(BF16).reshape(lead + value.shape[-1:])


def norm_into(r, l, src, normed, rstd_ref, gain, shift, out):
    def body(rows, carry):
        s = src[rows, :]
        centre = s - jnp.mean(s, -1, keepdims=True)
        rstd = lax.rsqrt(jnp.mean(centre * centre, -1, keepdims=True) + EPS)
        n = centre * rstd
        normed[l, rows, :] = n
        rstd_ref[l, rows, :] = rstd
        out[rows, :] = (n * gain[l] + shift[l]).astype(BF16)
        return carry

    row_loop(body, 0)


def norm_back(r, l, grad_y, normed, rstd_ref, gain, base, out, out_low):
    def body(rows, carry):
        gain_sum, shift_sum, out_sum = carry
        gy = grad_y[rows, :]
        n = normed[l, rows, :]
        e = gy * gain[l]
        back = rstd_ref[l, rows, :] * (
            e - jnp.mean(e, -1, keepdims=True) - n * jnp.mean(e * n, -1, keepdims=True)
        )
        res = base[rows, :] + back
        out[rows, :] = res
        out_low[rows, :] = res.astype(BF16)
        return (
            gain_sum + jnp.sum(gy * n, 0, keepdims=True),
            shift_sum + jnp.sum(gy, 0, keepdims=True),
            out_sum + jnp.sum(res, 0, keepdims=True),
        )

    zero = jnp.zeros((1, D), F32)
    return row_loop(body, (zero, zero, zero))


def to_windows(r, l):
    tok = lax.broadcasted_iota(jnp.int32, (WROWS, ROWS), 1)
    return jnp.where(tok == r.idx_col[l], 1.0, 0.0).astype(BF16)


def to_grid(r, l):
    tok = lax.broadcasted_iota(jnp.int32, (ROWS, WROWS), 0)
    return jnp.where(tok == r.idx_row[l], 1.0, 0.0).astype(BF16)


def cell_place(j):
    return (2 * WIN - 1) * (j // WIN) + j % WIN


def cell_pick(shape, cell_axis):
    cell = lax.broadcasted_iota(jnp.int32, shape, cell_axis)
    place = lax.broadcasted_iota(jnp.int32, shape, 1 - cell_axis)
    row = lax.shift_right_logical(cell * 37, 8)
    hit = (place == cell + 6 * row) & (cell < CELLS)
    return jnp.where(hit, 1.0, 0.0)


def dot_exact(a, b):
    return lax.dot_general(
        a, b, (((1,), (0,)), ((), ())), precision=lax.Precision.HIGHEST, preferred_element_type=F32
    )


LAST_PLACE = cell_place(CELLS - 1)


def expand_bias(r, l):
    pick = cell_pick((128, PADC), 1)
    live = lax.broadcasted_iota(jnp.int32, (PADC, PADC), 0) < CELLS
    r.ES[...] = jnp.zeros_like(r.ES)
    for x in range(2):
        table = r.SM[x, l, 8:16, :HALF]
        for j in range(CELLS):
            turn = (HALF - (LAST_PLACE - cell_place(j))) % HALF
            turned = pltpu.roll(table, turn, 1) if turn else table
            r.ES[j, 8 * x : 8 * x + 8, :] = turned[:, :128]
    for h in range(16):
        square = dot_exact(r.ES[:, h, :], pick)
        r.bias[l, h // 4, :, (h % 4) * PADC : (h % 4 + 1) * PADC] = jnp.where(live, square, MASKED)


def table_grads(r, l):
    pick = cell_pick((PADC, 128), 0)
    for h in range(16):
        part = r.DS[h // 4, :, (h % 4) * PADC : (h % 4 + 1) * PADC]
        r.ES[:, h, :] = dot_exact(part, pick)
    total = jnp.zeros((16, HALF), F32)
    zero = jnp.zeros((16, 128), F32)
    for j in range(CELLS):
        wide = jnp.concatenate([r.ES[j], zero], axis=1)
        turn = LAST_PLACE - cell_place(j)
        total = total + (pltpu.roll(wide, turn, 1) if turn else wide)
    r.AR[l, 16:32, :HALF] = total
    r.AR[l, 16:32, HALF:] = jnp.zeros((16, HALF), F32)


def attention_forward(r, l):
    def window(w, carry):
        rows = pl.ds(pl.multiple_of(w * PADC, PADC), PADC)
        pos = lax.rem(w, 4)
        same = r.reg_col[l, pos] == r.reg_row[l, pos]
        for g in range(4):
            lanes = slice(g * 128, (g + 1) * 128)
            q, k, v = r.Q[l, rows, lanes], r.K[l, rows, lanes], r.V[l, rows, lanes]
            s = dot_nt(k, spread_heads(q)) + r.bias[l, g]
            s = jnp.where(same, s, MASKED)
            e = jnp.exp(s - jnp.max(s, 0, keepdims=True))
            p = (e / jnp.sum(e, 0, keepdims=True)).astype(BF16)
            r.PR[l, w * 4 + g] = p
            r.AW[rows, lanes] = gather_heads(dot_tn(p, v)).astype(BF16)
        return carry

    lax.fori_loop(0, OWN * 4, window, 0)


def attention_backward(r, l, during):
    zero = jnp.zeros((1, 128), F32)

    def window(w, carry):
        during(w)
        rows = pl.ds(pl.multiple_of(w * PADC, PADC), PADC)
        sums = list(carry)
        for g in range(4):
            lanes = slice(g * 128, (g + 1) * 128)
            q, k, v = r.Q[l, rows, lanes], r.K[l, rows, lanes], r.V[l, rows, lanes]
            da = r.AW[rows, lanes]
            p = r.PR[l, w * 4 + g]
            da_spread = spread_heads(da)
            pf = p.astype(F32)
            pg = dot_nt(v, da_spread)
            ds = pf * (pg - jnp.sum(pf * pg, 0, keepdims=True))
            r.DS[g] += ds
            low = ds.astype(BF16)
            dv = dot(p, da_spread)
            dk = dot(low, spread_heads(q))
            dq = gather_heads(dot_tn(low, k)) * SCALE_Q
            r.Q[l, rows, lanes] = dq.astype(BF16)
            r.K[l, rows, lanes] = dk.astype(BF16)
            r.V[l, rows, lanes] = dv.astype(BF16)
            sums[g] = sums[g] + jnp.sum(dq, 0, keepdims=True)
            sums[4 + g] = sums[4 + g] + jnp.sum(dv, 0, keepdims=True)
        return tuple(sums)

    return lax.fori_loop(0, OWN * 4, window, (zero,) * 8)


def skip(*args):
    return None


IDLE = types.SimpleNamespace(need=skip, mlp=skip, mlp_done=skip, window=skip, attention_done=skip)


def forward(r, l, hooks):
    norm_into(r, l, r.S, r.N1, r.R1, r.ln1_gain, r.ln1_bias, r.YB)
    r.YW[l] = dot(to_windows(r, l), r.YB[...]).astype(BF16)
    hooks.need(l, 0)
    yw = r.YW[l]
    for x in range(2):
        cols = slice(x * HALF, (x + 1) * HALF)
        q = dot(yw, weight(r, l, 0, x, slice(0, HALF)))
        r.Q[l, :, cols] = ((q + r.SM[x, l, 1:2, :HALF]) * SCALE_Q).astype(BF16)
        r.K[l, :, cols] = dot(yw, weight(r, l, 0, x, slice(HALF, 2 * HALF))).astype(BF16)
        v = dot(yw, weight(r, l, 0, x, slice(2 * HALF, 3 * HALF)))
        r.V[l, :, cols] = (v + r.SM[x, l, 1:2, HALF : 2 * HALF]).astype(BF16)
    attention_forward(r, l)
    r.AT[l] = dot(to_grid(r, l), r.AW[...]).astype(BF16)
    for n in range(2):
        cols = slice(n * HALF, (n + 1) * HALF)
        acc = dot_nt(r.AT[l, :, :HALF], weight_rows(r, l, 0, 0, n, slice(3 * HALF, 4 * HALF)))
        acc += dot_nt(r.AT[l, :, HALF:], weight_rows(r, l, 0, 1, n, slice(3 * HALF, 4 * HALF)))
        r.S[:, cols] = r.S[:, cols] + acc + r.proj_bias[l, :, cols]
    norm_into(r, l, r.S, r.N2, r.R2, r.ln2_gain, r.ln2_bias, r.YB)
    r.Y2[l] = r.YB[...]
    hooks.need(l, 1)
    for x in range(2):

        def up(n, carry):
            at = pl.ds(pl.multiple_of(n * HALF, HALF), HALF)
            full = pl.ds(pl.multiple_of(x * 1024 + n * HALF, HALF), HALF)
            pre = dot(r.YB[...], weight(r, l, 1, x, at)) + r.SM[x, l, 0:1, at]
            phi = 0.5 * (1.0 + lax.erf(pre * INV_ROOT_TWO))
            r.AC[l, :, full] = (pre * phi).astype(BF16)
            dens = jnp.exp(-0.5 * pre * pre) * INV_ROOT_TWOPI
            r.SL[l, :, full] = (phi + pre * dens).astype(BF16)
            return carry

        lax.fori_loop(0, 4, up, 0)
    hooks.need(l, 2)
    for n in range(2):
        cols = slice(n * HALF, (n + 1) * HALF)
        acc = dot_nt(r.AC[l, :, :1024], weight_rows(r, l, 2, 0, n, slice(0, 1024)))
        acc += dot_nt(r.AC[l, :, 1024:], weight_rows(r, l, 2, 1, n, slice(0, 1024)))
        r.S[:, cols] = r.S[:, cols] + acc + r.fc2_bias[l, :, cols]


def backward_mlp(r, l, hooks):
    def low(rows, total):
        g = r.S[rows, :]
        r.YB[rows, :] = g.astype(BF16)
        return total + jnp.sum(g, 0, keepdims=True)

    r.AR[l, 9:10, :] = row_loop(low, jnp.zeros((1, D), F32))
    r.TA[...] = r.YB[...].T
    r.TB[:, :ROWS] = r.Y2[l].T
    for x in range(2):

        def down(n, carry):
            hooks.mlp(l, x * 4 + n)
            at = pl.ds(pl.multiple_of(n * HALF, HALF), HALF)
            full = pl.ds(pl.multiple_of(x * 1024 + n * HALF, HALF), HALF)
            pg = dot(r.YB[...], weight(r, l, 2, x, at)) * r.SL[l, :, full].astype(F32)
            r.F1[0:1, full] = jnp.sum(pg, 0, keepdims=True)
            pb = pg.astype(BF16)
            r.SL[l, :, full] = pb
            put_grad(r, l, 2, x, at, dot(r.TA[...], r.AC[l, :, full]))
            put_grad(r, l, 1, x, at, dot(r.TB[:, :ROWS], pb))
            return carry

        lax.fori_loop(0, 4, down, 0)
    hooks.mlp_done(l)
    for row in range(4):
        r.AR[l, row : row + 1, :] = r.F1[0:1, row * D : (row + 1) * D]
    for n in range(2):
        cols = slice(n * HALF, (n + 1) * HALF)
        acc = dot_nt(r.SL[l, :, :1024], weight_rows(r, l, 1, 0, n, slice(0, 1024)))
        acc += dot_nt(r.SL[l, :, 1024:], weight_rows(r, l, 1, 1, n, slice(0, 1024)))
        r.GY[:, cols] = acc
    gain, shift, out = norm_back(r, l, r.GY, r.N2, r.R2, r.ln2_gain, r.S, r.S, r.YB)
    r.AR[l, 6:7, :] = gain
    r.AR[l, 7:8, :] = shift
    r.AR[l, 8:9, :] = out


def backward_attention(r, l, hooks):
    r.TA[...] = r.YB[...].T
    for x in range(2):
        cols = slice(x * HALF, (x + 1) * HALF)
        put_grad(r, l, 0, x, slice(3 * HALF, 4 * HALF), dot(r.TA[...], r.AT[l, :, cols]))
        att = dot(r.YB[...], weight(r, l, 0, x, slice(3 * HALF, 4 * HALF)))
        r.GB[:, cols] = att.astype(BF16)
    r.AW[...] = dot(to_windows(r, l), r.GB[...]).astype(BF16)
    r.DS[...] = jnp.zeros_like(r.DS)
    sums = attention_backward(r, l, lambda w: hooks.window(l, w))
    for g in range(4):
        r.AR[l, 10:11, g * 128 : (g + 1) * 128] = sums[g]
        r.AR[l, 11:12, g * 128 : (g + 1) * 128] = sums[4 + g]
    r.AR[l, 12:16, :] = jnp.zeros((4, D), F32)
    r.TB[...] = r.YW[l].T
    for x in range(2):
        half = slice(x * HALF, (x + 1) * HALF)
        for part, ref in enumerate((r.Q, r.K, r.V)):
            cols = slice(part * HALF, (part + 1) * HALF)
            put_grad(r, l, 0, x, cols, dot(r.TB[...], ref[l, :, half]))
    hooks.attention_done(l)
    for n in range(2):
        cols = slice(n * HALF, (n + 1) * HALF)
        acc = jnp.zeros((WROWS, HALF), F32)
        for x in range(2):
            half = slice(x * HALF, (x + 1) * HALF)
            for part, ref in enumerate((r.Q, r.K, r.V)):
                take = slice(part * HALF, (part + 1) * HALF)
                acc += dot_nt(ref[l, :, half], weight_rows(r, l, 0, x, n, take))
        r.AW[:, cols] = acc.astype(BF16)
    r.GY[...] = dot(to_grid(r, l), r.AW[...])
    gain, shift, _ = norm_back(r, l, r.GY, r.N1, r.R1, r.ln1_gain, r.S, r.S, r.YB)
    r.AR[l, 4:5, :] = gain
    r.AR[l, 5:6, :] = shift
    table_grads(r, l)


ROW_INPUTS = ("ln1_gain", "ln1_bias", "proj_bias", "ln2_gain", "ln2_bias", "fc2_bias")
INPUTS = ("x", "cot", "valid", "idx_col", "idx_row", "reg_col", "reg_row") + ROW_INPUTS
SMALL = 32


def scratch_spec():
    return dict(
        S=pltpu.VMEM((ROWS, D), F32),
        GY=pltpu.VMEM((ROWS, D), F32),
        YB=pltpu.VMEM((ROWS, D), BF16),
        GB=pltpu.VMEM((ROWS, D), BF16),
        N1=pltpu.VMEM((LAYERS, ROWS, D), F32),
        N2=pltpu.VMEM((LAYERS, ROWS, D), F32),
        R1=pltpu.VMEM((LAYERS, ROWS, 1), F32),
        R2=pltpu.VMEM((LAYERS, ROWS, 1), F32),
        YW=pltpu.VMEM((LAYERS, WROWS, D), BF16),
        Q=pltpu.VMEM((LAYERS, WROWS, D), BF16),
        K=pltpu.VMEM((LAYERS, WROWS, D), BF16),
        V=pltpu.VMEM((LAYERS, WROWS, D), BF16),
        PR=pltpu.VMEM((LAYERS, OWN * 16, PADC, 4 * PADC), BF16),
        AW=pltpu.VMEM((WROWS, D), BF16),
        AT=pltpu.VMEM((LAYERS, ROWS, D), BF16),
        Y2=pltpu.VMEM((LAYERS, ROWS, D), BF16),
        AC=pltpu.VMEM((LAYERS, ROWS, FF), BF16),
        SL=pltpu.VMEM((LAYERS, ROWS, FF), BF16),
        TA=pltpu.VMEM((D, ROWS), BF16),
        TB=pltpu.VMEM((D, WROWS), BF16),
        ES=pltpu.VMEM((PADC, 16, 128), F32),
        DS=pltpu.VMEM((4, PADC, 4 * PADC), F32),
        bias=pltpu.VMEM((LAYERS, 4, PADC, 4 * PADC), F32),
        F1=pltpu.VMEM((1, FF), F32),
    )


def plain_kernel(names, *refs):
    r = types.SimpleNamespace(**dict(zip(names, refs)))
    r.S[...] = r.x[...].astype(F32)

    def ahead(l, c):
        expand_bias(r, l)
        forward(r, l, IDLE)
        return c

    lax.fori_loop(0, LAYERS, ahead, 0)
    r.result[...] = (r.S[...] * r.valid[...]).astype(BF16)
    r.S[...] = r.cot[...].astype(F32) * r.valid[...]

    def back(i, c):
        l = LAYERS - 1 - i
        backward_mlp(r, l, IDLE)
        backward_attention(r, l, IDLE)
        return c

    lax.fori_loop(0, LAYERS, back, 0)
    r.gimg[...] = r.YB[...]


def vmem_specs(n):
    return [pl.BlockSpec(memory_space=pltpu.VMEM)] * n


def plain_call(ins, small, w):
    outs = dict(
        G=jax.ShapeDtypeStruct(w.shape, BF16),
        AR=jax.ShapeDtypeStruct((LAYERS, SMALL, D), F32),
        result=jax.ShapeDtypeStruct((ROWS, D), BF16),
        gimg=jax.ShapeDtypeStruct((ROWS, D), BF16),
    )
    scratch = scratch_spec()
    names = INPUTS + ("SM", "W") + tuple(outs) + tuple(scratch)
    got = pl.pallas_call(
        functools.partial(plain_kernel, names),
        out_shape=list(outs.values()),
        in_specs=vmem_specs(len(INPUTS) + 2),
        out_specs=vmem_specs(len(outs)),
        scratch_shapes=list(scratch.values()),
        compiler_params=pltpu.CompilerParams(vmem_limit_bytes=67043328),
        name="step",
    )(*[ins[name] for name in INPUTS], small, w)
    return dict(zip(outs, got))


def kernel_inputs(images, cot, load, mp, rows):
    idx, reg = token_maps()
    keep = OWN * TOK_IMG

    def own(arr):
        slots = lax.dynamic_slice_in_dim(arr.swapaxes(0, 1), mp * OWN, OWN, 1)
        return jnp.pad(slots.reshape(keep, D), ((0, ROWS - keep), (0, 0)))

    at = jnp.arange(ROWS, dtype=jnp.int32)
    live = (mp * OWN + at % OWN < load) & (at < keep)
    ins = dict(
        x=own(images), cot=own(cot), valid=live.astype(F32)[:, None],
        idx_col=jnp.asarray(idx)[:, :, None], idx_row=jnp.asarray(idx)[:, None, :],
        reg_col=jnp.asarray(reg)[:, :, :, None],
        reg_row=jnp.asarray(np.tile(reg, (1, 1, 4)))[:, :, None, :],
    )
    ins.update({name: a.reshape(LAYERS, 1, -1) for name, a in rows.items()})
    return ins


def pack_small(fc1_bias, qv_bias, rel_table):
    wide = lambda a: jnp.pad(a, ((0, 0), (0, 0), (0, 1024 - a.shape[2])))
    return jnp.concatenate(
        [
            fc1_bias.reshape(LAYERS, 1, 1024),
            wide(qv_bias.reshape(LAYERS, 1, 2 * HALF)),
            jnp.zeros((LAYERS, 6, 1024), F32),
            wide(rel_table),
        ],
        1,
    )


def pack_weights(w_qkv, w_proj, w_fc1, w_fc2):
    rows = w_qkv.shape[1]
    first = jnp.concatenate([w_qkv.reshape(LAYERS, rows, -1), w_proj.swapaxes(1, 2)], 2)
    return jnp.stack([first, w_fc1, w_fc2.swapaxes(1, 2)], 1)


MESH = pl.DeviceIdType.MESH
UNITS = 3 * LAYERS
Z_SIDE = 4


class Place:
    def __init__(self):
        self.dp = lax.axis_index("dp")
        self.x = lax.axis_index("mp")
        self.c = lax.rem(self.dp, 2)
        self.y = lax.rem(self.dp // 2, 2)
        self.z = self.dp // 4
        self.sib = {"dp": self.dp + 1 - 2 * self.c, "mp": self.x}
        self.ynbr = {"dp": self.dp + 2 - 4 * self.y, "mp": self.x}
        self.xnbr = {"dp": self.dp, "mp": 1 - self.x}

    def zpos(self, k):
        return lax.rem(self.z + k, Z_SIDE)

    def zpeer(self, k):
        return {"dp": self.zpos(k) * 4 + lax.rem(self.dp, 4), "mp": self.x}

    def peers(self):
        return [self.sib, self.ynbr, self.xnbr] + [self.zpeer(k) for k in range(1, Z_SIDE)]


def greet(place):
    barrier = pltpu.get_barrier_semaphore()
    peers = place.peers()
    for peer in peers:
        pl.semaphore_signal(barrier, inc=1, device_id=peer, device_id_type=MESH)
    pl.semaphore_wait(barrier, len(peers))


def remote(src, dst, sems, u, k, peer):
    return pltpu.make_async_remote_copy(
        src_ref=src, dst_ref=dst, send_sem=sems.at[0, u, k], recv_sem=sems.at[1, u, k],
        device_id=peer, device_id_type=MESH,
    )


def landed(dst, sems, u, k, peer):
    remote(dst, dst, sems, u, k, peer).wait_recv()


TOP, LOW = pl.ds(0, 16), pl.ds(16, 16)


class Gather:
    def __init__(self, place, shard, w, sems, local):
        self.p, self.shard, self.w, self.sems, self.local = place, shard, w, sems, local

    def slab(self, u, x, y, c, part=None):
        ref = self.w.at[u // 3, lax.rem(u, 3), x, :, y, c]
        return ref if part is None else ref.at[:, part]

    def block(self, u, z):
        p = self.p
        return self.w.at[u // 3, lax.rem(u, 3), p.x, z, p.y, p.c]

    def own(self, u):
        return self.shard.at[u // 3, lax.rem(u, 3)]

    def z_copy(self, u, k):
        return remote(self.own(u), self.block(u, self.p.z), self.sems, u, k - 1, self.p.zpeer(k))

    def local_copy(self, u):
        return pltpu.make_async_copy(self.own(u), self.block(u, self.p.z), self.local.at[u])

    def full_copies(self, u):
        p = self.p
        mine = self.slab(u, p.x, p.y, p.c)
        return [
            remote(mine, mine, self.sems, u, 3, p.xnbr),
            remote(mine, mine, self.sems, u, 4, p.ynbr),
            remote(mine, mine, self.sems, u, 5, p.sib),
        ]

    def half_copies(self, u):
        p = self.p
        from_y, from_x = (p.x, 1 - p.y, p.c), (1 - p.x, p.y, p.c)
        top, low = self.slab(u, *from_y, TOP), self.slab(u, *from_x, LOW)
        fy, fx = self.slab(u, *from_y), self.slab(u, *from_x)
        return [
            remote(top, top, self.sems, u, 6, p.xnbr),
            remote(low, low, self.sems, u, 7, p.ynbr),
            remote(fx, fx, self.sems, u, 8, p.sib),
            remote(fy, fy, self.sems, u, 9, p.sib),
        ]

    def last_copies(self, u):
        p = self.p
        far = self.slab(u, 1 - p.x, 1 - p.y, p.c)
        return [remote(far, far, self.sems, u, 10, p.sib)]

    def start_own(self, u):
        self.local_copy(u).start()
        for k in range(1, Z_SIDE):
            self.z_copy(u, k).start()

    def pass_own(self, u):
        p = self.p
        self.local_copy(u).wait()
        for k in range(1, Z_SIDE):
            landed(self.block(u, p.zpos(Z_SIDE - k)), self.sems, u, k - 1, p.zpeer(Z_SIDE - k))
        for copy in self.full_copies(u):
            copy.start()

    def pass_near(self, u):
        p = self.p
        landed(self.slab(u, 1 - p.x, p.y, p.c), self.sems, u, 3, p.xnbr)
        landed(self.slab(u, p.x, 1 - p.y, p.c), self.sems, u, 4, p.ynbr)
        for copy in self.half_copies(u):
            copy.start()

    def pass_far(self, u):
        p = self.p
        landed(self.slab(u, 1 - p.x, 1 - p.y, p.c, TOP), self.sems, u, 6, p.xnbr)
        landed(self.slab(u, 1 - p.x, 1 - p.y, p.c, LOW), self.sems, u, 7, p.ynbr)
        for copy in self.last_copies(u):
            copy.start()

    def ready(self, u):
        p = self.p
        for k, (x, y) in ((5, (p.x, p.y)), (8, (1 - p.x, p.y)), (9, (p.x, 1 - p.y)), (10, (1 - p.x, 1 - p.y))):
            landed(self.slab(u, x, y, 1 - p.c), self.sems, u, k, p.sib)

    def tick(self, t):
        @pl.when(t < UNITS)
        def _():
            self.pass_own(t)

        @pl.when(t + 2 < UNITS)
        def _():
            self.start_own(t + 2)

        @pl.when((t >= 1) & (t - 1 < UNITS))
        def _():
            self.pass_near(t - 1)

        @pl.when((t >= 2) & (t - 2 < UNITS))
        def _():
            self.pass_far(t - 2)

    def drain(self, u):
        for k in range(1, Z_SIDE):
            self.z_copy(u, k).wait_send()
        for copy in self.full_copies(u) + self.half_copies(u) + self.last_copies(u):
            copy.wait_send()


class Scatter:
    def __init__(self, place, r):
        self.p, self.r, self.sems = place, r, r.sums

    def buf(self, ref, u):
        return ref.at[lax.rem(u, 3)]

    def grads(self, u):
        return self.r.G.at[u // 3, lax.rem(u, 3)]

    def sib_copy(self, u):
        p = self.p
        src = self.grads(u).at[:, :, :, 1 - p.c]
        return remote(src, self.buf(self.r.P, u), self.sems, u, 0, p.sib)

    def part(self, u, x, y, rows=None):
        ref = self.buf(self.r.P, u).at[x, :, y]
        return ref if rows is None else ref.at[:, rows]

    def far_copies(self, u):
        p, into = self.p, self.buf(self.r.RA, u)
        return [
            remote(self.part(u, 1 - p.x, 1 - p.y, TOP), into.at[0], self.sems, u, 1, p.xnbr),
            remote(self.part(u, 1 - p.x, 1 - p.y, LOW), into.at[1], self.sems, u, 2, p.ynbr),
        ]

    def near_copies(self, u):
        p, into = self.p, self.buf(self.r.RB, u)
        return [
            remote(self.part(u, 1 - p.x, p.y), into.at[0], self.sems, u, 3, p.xnbr),
            remote(self.part(u, p.x, 1 - p.y), into.at[1], self.sems, u, 4, p.ynbr),
        ]

    def z_copy(self, u, k):
        p = self.p
        src = self.buf(self.r.P, u).at[p.x, p.zpos(k), p.y]
        return remote(src, self.buf(self.r.RC, u).at[k - 1], self.sems, u, 4 + k, p.zpeer(k))

    def add(self, dst, *srcs):
        def step(z, c):
            total = dst[z].astype(F32)
            for src in srcs:
                total = total + src[z].astype(F32)
            dst[z] = total.astype(BF16)
            return c

        lax.fori_loop(0, Z_SIDE, step, 0)

    def sib(self, u):
        self.sib_copy(u).start()

    def far(self, u):
        p = self.p
        landed(self.buf(self.r.P, u), self.sems, u, 0, p.sib)
        grads = self.grads(u)
        self.add(self.part(u, 1 - p.x, 1 - p.y), grads.at[1 - p.x, :, 1 - p.y, p.c])
        for copy in self.far_copies(u):
            copy.start()
        for x, y in ((1 - p.x, p.y), (p.x, 1 - p.y), (p.x, p.y)):
            self.add(self.part(u, x, y), grads.at[x, :, y, p.c])

    def near(self, u):
        p, got = self.p, self.buf(self.r.RA, u)
        landed(got.at[0], self.sems, u, 1, p.xnbr)
        landed(got.at[1], self.sems, u, 2, p.ynbr)
        self.add(self.part(u, p.x, 1 - p.y, TOP), got.at[0])
        self.add(self.part(u, 1 - p.x, p.y, LOW), got.at[1])
        for copy in self.near_copies(u):
            copy.start()

    def z(self, u):
        p, got = self.p, self.buf(self.r.RB, u)
        landed(got.at[0], self.sems, u, 3, p.xnbr)
        landed(got.at[1], self.sems, u, 4, p.ynbr)
        self.add(self.part(u, p.x, p.y), got.at[0], got.at[1])
        for k in range(1, Z_SIDE):
            self.z_copy(u, k).start()

    def finish(self, u):
        p, r = self.p, self.r
        total = r.P[lax.rem(u, 3), p.x, p.z, p.y].astype(F32)
        for k in range(1, Z_SIDE):
            landed(self.buf(r.RC, u).at[k - 1], self.sems, u, 4 + k, p.zpeer(Z_SIDE - k))
            total = total + r.RC[lax.rem(u, 3), k - 1].astype(F32)
        r.grad[u // 3, lax.rem(u, 3)] = total
        for copy in [self.sib_copy(u)] + self.far_copies(u) + self.near_copies(u):
            copy.wait_send()
        for k in range(1, Z_SIDE):
            self.z_copy(u, k).wait_send()

    def release(self, g):
        for peer in self.p.peers():
            pl.semaphore_signal(self.r.free.at[g], inc=1, device_id=peer, device_id_type=MESH)

    def claim(self, g):
        pl.semaphore_wait(self.r.free.at[g], len(self.p.peers()))


class Total:
    def __init__(self, place, r):
        self.p, self.r, self.sems = place, r, r.totals

    def copy(self, l, k):
        p, r = self.p, self.r
        if k < 3:
            src = r.AR.at[l] if k == 0 else r.AS.at[l, k - 1]
            return remote(src, r.AB.at[l, k], self.sems, l, k, (p.sib, p.xnbr, p.ynbr)[k])
        hop = k - 2
        return remote(r.AS.at[l, 2], r.AZ.at[l, p.z], self.sems, l, k, p.zpeer(hop))

    def step(self, l, k):
        p, r = self.p, self.r
        if k:
            landed(r.AB.at[l, k - 1], self.sems, l, k - 1, (p.sib, p.xnbr, p.ynbr)[k - 1])
            mine = r.AR[l] if k == 1 else r.AS[l, k - 2]
            total = mine + r.AB[l, k - 1]
            r.AS[l, k - 1] = total
        if k < 3:
            self.copy(l, k).start()
        else:
            r.AZ[l, p.z] = total
            for hop in range(1, Z_SIDE):
                self.copy(l, 2 + hop).start()

    def finish(self, l):
        p, r = self.p, self.r
        for hop in range(1, Z_SIDE):
            from_z = p.zpos(Z_SIDE - hop)
            landed(r.AZ.at[l, from_z], self.sems, l, 2 + hop, p.zpeer(Z_SIDE - hop))
        total = r.AZ[l, 0]
        for z in range(1, Z_SIDE):
            total = total + r.AZ[l, z]
        r.small_sum[l] = total
        for k in range(2 + Z_SIDE):
            self.copy(l, k).wait_send()


def comm_scratch():
    return dict(
        W=pltpu.VMEM((LAYERS, 3, 2, Z_SIDE, 2, 2, 32, 1024), BF16),
        G=pltpu.VMEM((LAYERS, 3, 2, Z_SIDE, 2, 2, 32, 1024), BF16),
        P=pltpu.VMEM((3, 2, Z_SIDE, 2, 32, 1024), BF16),
        RA=pltpu.VMEM((3, 2, Z_SIDE, 16, 1024), BF16),
        RB=pltpu.VMEM((3, 2, Z_SIDE, 32, 1024), BF16),
        RC=pltpu.VMEM((3, Z_SIDE - 1, 32, 1024), BF16),
        SM=pltpu.VMEM((2, LAYERS, 16, 1024), F32),
        AR=pltpu.VMEM((LAYERS, SMALL, D), F32),
        AB=pltpu.VMEM((LAYERS, 3, SMALL, D), F32),
        AS=pltpu.VMEM((LAYERS, 3, SMALL, D), F32),
        AZ=pltpu.VMEM((LAYERS, Z_SIDE, SMALL, D), F32),
        gathers=pltpu.SemaphoreType.DMA((2, UNITS, 11)),
        local=pltpu.SemaphoreType.DMA((UNITS + 1,)),
        sums=pltpu.SemaphoreType.DMA((2, UNITS, 8)),
        totals=pltpu.SemaphoreType.DMA((2, LAYERS, 6)),
        swaps=pltpu.SemaphoreType.DMA((2, 1, 3)),
        free=pltpu.SemaphoreType.REGULAR((3,)),
    )


def fused_kernel(names, *refs):
    r = types.SimpleNamespace(**dict(zip(names, refs)))
    place = Place()
    x = place.x
    gather = Gather(place, r.shard, r.W, r.gathers, r.local)
    scatter = Scatter(place, r)
    total = Total(place, r)

    def swap(src, ref, k):
        return remote(src, ref.at[x], r.swaps, 0, k, place.xnbr)

    greet(place)
    gather.start_own(0)
    swap(r.small, r.SM, 0).start()
    own_small = pltpu.make_async_copy(r.small, r.SM.at[x], r.local.at[UNITS])
    own_small.start()
    gather.start_own(1)
    r.S[...] = r.x[...].astype(F32)
    own_small.wait()
    landed(r.SM.at[1 - x], r.swaps, 0, 0, place.xnbr)
    swap(r.small, r.SM, 0).wait_send()

    def opening(l, c):
        gather.tick(l)
        expand_bias(r, l)
        return c

    lax.fori_loop(0, LAYERS, opening, 0)

    def need(l, g):
        gather.tick(3 * l + g + 2)
        gather.ready(3 * l + g)

    ahead = types.SimpleNamespace(need=need)

    def forward_step(l, c):
        forward(r, l, ahead)
        return c

    lax.fori_loop(0, LAYERS, forward_step, 0)
    r.result[x] = (r.S[...] * r.valid[...]).astype(BF16)
    r.S[...] = r.cot[...].astype(F32) * r.valid[...]

    def drain(u, c):
        gather.drain(u)
        return c

    lax.fori_loop(0, UNITS, drain, 0)
    swap(r.result.at[x], r.result, 1).start()

    def at(cond, *acts):
        @pl.when(cond)
        def _():
            for act in acts:
                act()

    def mlp(l, k):
        low = l == 0
        at(low & (k == 1), lambda: scatter.finish(5), lambda: scatter.release(2))
        at(low & (k == 2), lambda: scatter.near(3))
        at(low & (k == 3), lambda: scatter.finish(4), lambda: scatter.release(1))
        at(low & (k == 4), lambda: total.step(1, 1))
        at(low & (k == 6), lambda: total.step(1, 2))

    def mlp_done(l):
        at(l == 0, lambda: scatter.z(3), lambda: scatter.claim(2))
        scatter.sib(3 * l + 2)
        at(l == 0, lambda: scatter.claim(1))
        scatter.sib(3 * l + 1)

    def window(l, w):
        low = l == 0
        at(w == 0, lambda: scatter.far(3 * l + 2))
        at(low & (w == 1), lambda: total.step(1, 3))
        at(w == 2, lambda: scatter.far(3 * l + 1))
        at(low & (w == 3), lambda: scatter.finish(3), lambda: scatter.release(0))
        at(w == 4, lambda: scatter.near(3 * l + 2))
        at(low & (w == 5), lambda: total.finish(1))
        at(w == 7, lambda: scatter.near(3 * l + 1))

    def attention_done(l):
        at(l == 0, lambda: scatter.claim(0))
        scatter.sib(3 * l)
        scatter.z(3 * l + 2)

    hooks = types.SimpleNamespace(
        mlp=mlp, mlp_done=mlp_done, window=window, attention_done=attention_done
    )

    def backward_step(i, c):
        l = LAYERS - 1 - i
        backward_mlp(r, l, hooks)
        backward_attention(r, l, hooks)
        scatter.z(3 * l + 1)
        scatter.far(3 * l)
        total.step(l, 0)
        return c

    lax.fori_loop(0, LAYERS, backward_step, 0)
    r.gimg[x] = r.YB[...]
    scatter.finish(2)
    scatter.near(0)
    swap(r.gimg.at[x], r.gimg, 2).start()
    total.step(0, 1)
    scatter.finish(1)
    total.step(0, 2)
    scatter.z(0)
    total.step(0, 3)
    scatter.finish(0)
    total.finish(0)
    for k, ref in ((1, r.result), (2, r.gimg)):
        landed(ref.at[1 - x], r.swaps, 0, k, place.xnbr)
        swap(ref.at[x], ref, k).wait_send()


def fused_call(ins, small, shard):
    outs = dict(
        grad=jax.ShapeDtypeStruct((LAYERS, 3, 32, 1024), F32),
        small_sum=jax.ShapeDtypeStruct((LAYERS, SMALL, D), F32),
        result=jax.ShapeDtypeStruct((2, ROWS, D), BF16),
        gimg=jax.ShapeDtypeStruct((2, ROWS, D), BF16),
    )
    scratch = scratch_spec() | comm_scratch()
    names = INPUTS + ("small", "shard") + tuple(outs) + tuple(scratch)
    got = pl.pallas_call(
        functools.partial(fused_kernel, names),
        out_shape=list(outs.values()),
        in_specs=vmem_specs(len(INPUTS) + 2),
        out_specs=vmem_specs(len(outs)),
        scratch_shapes=list(scratch.values()),
        compiler_params=pltpu.CompilerParams(
            collective_id=0, has_side_effects=True, vmem_limit_bytes=67043328
        ),
        name="step",
    )(*[ins[name] for name in INPUTS], small, shard)
    return dict(zip(outs, got))


def gather_plain(shard):
    full = lax.all_gather(shard, "dp", axis=2, tiled=True)
    return lax.all_gather(full, "mp", axis=2, tiled=False)


def scatter_plain(grad):
    half = lax.psum_scatter(grad, "mp", scatter_dimension=2, tiled=False)
    return lax.psum_scatter(half, "dp", scatter_dimension=2, tiled=True).astype(F32)


def collective_call(ins, small, shard):
    full = gather_plain(shard).reshape(LAYERS, 3, 2, 4, 1, 1, D // 4, 1024)
    outs = plain_call(ins, lax.all_gather(small, "mp"), full)
    return dict(
        grad=scatter_plain(outs["G"].reshape(LAYERS, 3, 2, D, 1024)),
        small_sum=lax.psum(outs["AR"], ("dp", "mp")),
        result=lax.all_gather(outs["result"], "mp"),
        gimg=lax.all_gather(outs["gimg"], "mp"),
    )


def per_device(
    images, loads, cotangent, ln1_gain, ln1_bias, w_qkv, qv_bias, rel_table, w_proj, proj_bias,
    ln2_gain, ln2_bias, w_fc1, fc1_bias, w_fc2, fc2_bias,
):
    mp = lax.axis_index("mp")
    rows = dict(
        ln1_gain=ln1_gain, ln1_bias=ln1_bias, proj_bias=proj_bias, ln2_gain=ln2_gain,
        ln2_bias=ln2_bias, fc2_bias=fc2_bias,
    )
    ins = kernel_inputs(images, cotangent, loads[0], mp, rows)
    small = pack_small(fc1_bias, qv_bias, rel_table)
    shard = pack_weights(w_qkv, w_proj, w_fc1, w_fc2)
    direct = lax.axis_size("dp") == 4 * Z_SIDE and lax.axis_size("mp") == 2
    outs = (fused_call if direct else collective_call)(ins, small, shard)
    grad, sums = outs["grad"], outs["small_sum"]

    def whole(both):
        kept = both[:, : OWN * TOK_IMG].reshape(2, TOK_IMG, OWN, D)
        return kept.transpose(0, 2, 1, 3).reshape(2 * OWN, TOK_IMG, D)

    entries = rel_table.shape[2]
    return (
        whole(outs["result"]),
        whole(outs["gimg"]),
        sums[:, 4],
        sums[:, 5],
        grad[:, 0, :, : 3 * HALF].reshape(w_qkv.shape),
        lax.dynamic_slice_in_dim(sums[:, 10:12], mp * HALF, HALF, 2),
        lax.dynamic_slice_in_dim(sums[:, 16:32], mp * 8, 8, 1)[:, :, :entries],
        grad[:, 0, :, 3 * HALF :].swapaxes(1, 2),
        sums[:, 8],
        sums[:, 6],
        sums[:, 7],
        grad[:, 1],
        lax.dynamic_slice_in_dim(sums[:, :4].reshape(LAYERS, FF), mp * 1024, 1024, 1),
        grad[:, 2].swapaxes(1, 2),
        sums[:, 9],
    )


def solution(mesh):
    wq, cols = P(None, "dp", None, "mp"), P(None, "mp")
    rows_dp, cols_dp = P(None, "dp", "mp"), P(None, "mp", "dp")
    img = P("dp", None, None)
    qv, tab = P(None, None, "mp"), P(None, "mp", None)
    return jax.shard_map(
        per_device,
        mesh=mesh,
        in_specs=(
            img, P("dp"), img, P(), P(), wq, qv, tab, cols_dp, P(), P(), P(), rows_dp, cols, cols_dp, P(),
        ),
        out_specs=(img, img, P(), P(), wq, qv, tab, cols_dp, P(), P(), P(), rows_dp, cols, cols_dp, P()),
        check_vma=False,
    )
```
